512 devices in a mesh: gx: 8 (over x, core), gy: 16 (over z), lev: 4 (over y).
Axes of the slice: x: 4, y: 4, z: 16, core: 2. Of those that a mesh axis runs over, the one named last changes fastest.
Arguments:
- zonal: float32 [128, 256, 2048], P('lev', 'gx', 'gy'), may hold values from -6 to 6
- meridional: float32 [128, 256, 2048], P('lev', 'gx', 'gy'), may hold values from -6 to 6
- vertical: float32 [128, 256, 2048], P('lev', 'gx', 'gy'), may hold values from -4 to 4
- pressure: float32 [128, 256, 2048], P('lev', 'gx', 'gy'), may hold values from -6 to 6
- coupling: float32 [128, 256, 2048], P('lev', 'gx', 'gy'), may hold values from 0.125 to 32768
- surface: int32 [256, 2048], P('gx', 'gy'), may hold values from 0 to 16
- lid_flag: int32 [256, 2048], P('gx', 'gy'), may hold values from 0 to 1
Outputs:
- zonal_out: float32 [128, 256, 2048], P('lev', 'gx', 'gy')
- meridional_out: float32 [128, 256, 2048], P('lev', 'gx', 'gy')
- vertical_out: float32 [128, 256, 2048], P('lev', 'gx', 'gy')
- pressure_out: float32 [128, 256, 2048], P('lev', 'gx', 'gy')
The draws below stay inside these ranges and needn't reach their ends.
Inputs may be any that keep to these rules, and one draw needn't show every extreme that they name: `surface`: the number of lowest levels of a column that lie below the terrain. `lid_flag`: 1 closes the column's top with a rigid lid, 0 leaves it open.
All inputs are finite; a program needn't handle non-finite values.
Results may differ from the reference program's by a relative error of at most 0.0003.
Values sent between devices are 32-bit elements; how exact they have to be, the bound alone decides.
A program may use at most 128 MiB of HBM per device.

```python
import math
import jax
import jax.numpy as jnp
from jax import lax

LZ = 32
SUBSTEPS = 3
NZ = 128
NX = 256
NY = 2048


def draw_vertical(key, part):
    values = jnp.clip(jax.random.normal(key, (NZ, NX, NY), jnp.float32), -4.0, 4.0)
    return values


def draw_coupling(key, part):
    column_key = jax.random.fold_in(key, 11)
    level_key = jax.random.fold_in(key, 23)
    column_high = math.log(16.0 * LZ * LZ)
    column_log = jax.random.uniform(column_key, (NX, NY), jnp.float32, math.log(0.25), column_high)
    column_scale = jnp.exp(column_log)
    rough_log = jax.random.uniform(level_key, (NZ, NX, NY), jnp.float32, math.log(0.5), math.log(2.0))
    rough = jnp.exp(rough_log)
    return column_scale[None] * rough


def touch_ends(drawn, stream_key, low, top_value):
    longest = drawn.shape.index(max(drawn.shape))
    spots = []
    for shift in (0, 1):
        where = [jax.random.randint(jax.random.fold_in(stream_key, axis), (), 0, length) for axis, length in enumerate(drawn.shape)]
        where[longest] = (where[longest] + shift) % drawn.shape[longest]
        spots.append(tuple(where))
    return drawn.at[spots[0]].set(low).at[spots[1]].set(top_value)


def level_of(own_key, dims, pieces, smallest, top_value):
    level, own = 1.0, jax.random.fold_in(own_key, 6)
    for dim, blocks in pieces:
        draws = jnp.exp(jax.random.uniform(jax.random.fold_in(own, dim), (blocks,), jnp.float32, smallest / len(pieces), top_value / len(pieces)))
        level = level * jnp.repeat(draws, dims[dim] // blocks).reshape([-1 if axis == dim else 1 for axis in range(len(dims))])
    return level


def centred(key, shape, scale, reach, cuts=(), dtype=jnp.bfloat16):
    result = scale * jax.random.normal(key, shape, jnp.float32)
    if cuts:
        result = result * level_of(key, shape, cuts, -0.22, 0.18)
    return jnp.clip(result, -reach, reach).astype(dtype)


def setup_inputs(seed: int = 0) -> dict:
    splits = jax.random.split(jax.random.key(seed), 8)
    return {
        "zonal": centred(splits[0], (NZ, NX, NY), 1.0, 6.0, ((0, 4), (1, 8), (2, 16)), jnp.float32),
        "meridional": centred(splits[1], (NZ, NX, NY), 1.0, 6.0, ((0, 4), (1, 8), (2, 16)), jnp.float32),
        "vertical": draw_vertical(jax.random.fold_in(splits[7], 71), 0),
        "pressure": centred(splits[3], (NZ, NX, NY), 1.0, 6.0, ((0, 4), (1, 8), (2, 16)), jnp.float32),
        "coupling": draw_coupling(jax.random.fold_in(splits[7], 71), 0),
        "surface": touch_ends(jax.random.randint(splits[5], (NX, NY), 0, LZ // 2 + 1), jax.random.fold_in(splits[5], 1), 0, (LZ // 2 + 1) - 1).astype(jnp.int32),
        "lid_flag": touch_ends(jax.random.randint(splits[6], (NX, NY), 0, 2), jax.random.fold_in(splits[6], 1), 0, 1).astype(jnp.int32),
    }


horizontal_step = 0.25
divergence_step = 0.25
vertical_step = 0.5
pressure_step = 0.5


def column_solve(lower, diagonal, upper, source):
    zeros_plane = jnp.zeros(diagonal.shape[1:], jnp.float32)

    def forward(state_pair, level_items):
        ratio_prev, part_prev = state_pair
        low_here, diag_here, up_here, source_here = level_items
        pivots = diag_here - low_here * ratio_prev
        ratio_new = up_here / pivots
        part_new = (source_here - low_here * part_prev) / pivots
        return (ratio_new, part_new), (ratio_new, part_new)

    unused, (ratios, parts) = lax.scan(forward, (zeros_plane, zeros_plane), (lower, diagonal, upper, source))

    def backward(value_next, level_items):
        ratio_here, part_here = level_items
        value = part_here - ratio_here * value_next
        return value, value

    unused_last, solution = lax.scan(backward, zeros_plane, (ratios, parts), reverse=True)
    return solution


def reference(zonal, meridional, vertical, pressure, coupling, surface, lid_flag):
    depth = coupling.shape[0]
    zeros_plane = jnp.zeros((1,) + coupling.shape[1:], jnp.float32)
    coupling_up = jnp.concatenate([coupling[1:], zeros_plane], 0)
    levels = lax.broadcasted_iota(jnp.int32, coupling.shape, 0)
    keep = levels >= surface[None]
    is_top = levels == depth - 1
    lid_value = lid_flag.astype(jnp.float32)[None]
    diagonal = 1.0 + coupling + coupling_up + jnp.where(is_top, lid_value * coupling, 0.0)
    lower = jnp.where(levels == 0, 0.0, -coupling)
    upper = -coupling_up
    diagonal = jnp.where(keep, diagonal, 1.0)
    lower = jnp.where(keep, lower, 0.0)
    upper = jnp.where(keep, upper, 0.0)
    for substep in range(SUBSTEPS):
        zonal = zonal - horizontal_step * (jnp.roll(pressure, -1, 1) - jnp.roll(pressure, 1, 1))
        meridional = meridional - horizontal_step * (jnp.roll(pressure, -1, 2) - jnp.roll(pressure, 1, 2))
        spread = (jnp.roll(zonal, -1, 1) - jnp.roll(zonal, 1, 1)) + (jnp.roll(meridional, -1, 2) - jnp.roll(meridional, 1, 2))
        partial_p = pressure - divergence_step * spread
        above_p = jnp.concatenate([partial_p[1:], zeros_plane], 0)
        below_p = jnp.concatenate([zeros_plane, partial_p[:-1]], 0)
        source = jnp.where(keep, vertical - vertical_step * (above_p - below_p), 0.0)
        vertical = column_solve(lower, diagonal, upper, source)
        previous = jnp.concatenate([zeros_plane, vertical[:-1]], 0)
        pressure = partial_p - pressure_step * (vertical - previous)
    return zonal, meridional, vertical, pressure
```

```python
import functools

import jax
import jax.numpy as jnp
from jax import lax
from jax.experimental import pallas as pl
from jax.experimental.pallas import tpu as pltpu
from jax.sharding import PartitionSpec as P

SUBSTEPS = 3
MESH = pl.DeviceIdType.MESH
PAD = 8


def kernel(
    zon, mer, ver, pre, cou, sur, lid,
    out_u, out_v, out_w, out_p,
    us, vs, ws, ps, cs, ks, ls,
    fs, pp, zz, am, im, gm, gf, gl,
    xs0, ys0, xs, ys, xr0, yr0, xr, yr,
    sta, lev, cup, pls, plr, inv,
    load_sem, store_sem, send_sem, recv_sem,
):
    L, I, J = zon.shape
    g = lax.axis_index("lev")
    gx = lax.axis_index("gx")
    gy = lax.axis_index("gy")
    groups = lax.axis_size("lev")
    nx = lax.axis_size("gx")
    ny = lax.axis_size("gy")
    x_lo = {"gx": lax.rem(gx + nx - 1, nx)}
    x_hi = {"gx": lax.rem(gx + 1, nx)}
    y_lo = {"gy": lax.rem(gy + ny - 1, ny)}
    y_hi = {"gy": lax.rem(gy + 1, ny)}
    peers = [{"lev": lax.rem(g + d, groups)} for d in range(1, groups)]
    inner = pl.ds(PAD, I)

    loads = [
        pltpu.make_async_copy(src, dst, load_sem.at[n])
        for n, (src, dst) in enumerate([
            (pre, ps.at[:, inner, :]),
            (mer, vs),
            (zon, us.at[:, inner, :]),
            (cou, cs.at[pl.ds(0, L)]),
            (sur, ks),
            (lid, ls),
            (ver, ws),
        ])
    ]
    for copy in loads:
        copy.start()
    barrier = pltpu.get_barrier_semaphore()
    everyone = [x_lo, x_hi, y_lo, y_hi] + peers
    for dev in everyone:
        pl.semaphore_signal(barrier, inc=1, device_id=dev, device_id_type=MESH)

    lane = lax.broadcasted_iota(jnp.int32, (I, J), 1)
    quad = lane // 4
    sub = lane % 4
    edge = (lane < 2) | (lane >= J - 2)
    zero = jnp.zeros((I, J), jnp.float32)

    def rows_out(src2, buf, side, at, row):
        buf[side, pl.ds(at * L, L), :] = src2[:, PAD + row, :]

    def rows_in(dst2, row, buf, side, at):
        dst2[:, PAD + row, :] = buf[side, pl.ds(at * L, L), :]

    sems = iter(range(64))

    def remote(src, dst, dev):
        n = next(sems)
        return pltpu.make_async_remote_copy(
            src_ref=src, dst_ref=dst, send_sem=send_sem.at[n], recv_sem=recv_sem.at[n],
            device_id=dev, device_id_type=MESH)

    loads[0].wait()
    loads[1].wait()
    loads[2].wait()
    for r in range(2):
        rows_out(ps, xs0, 0, r, r)
        rows_out(ps, xs0, 1, r, I - 2 + r)
    rows_out(us, xs0, 0, 2, 0)
    rows_out(us, xs0, 1, 2, I - 1)

    def pack0(k, held):
        a, b = held
        turn = 4 * k + 2
        mine = quad == k
        a = jnp.where(mine, pltpu.roll(ps[k, inner, :], turn, 1), a)
        b = jnp.where(mine, pltpu.roll(vs[k], turn, 1), b)
        return a, b

    pack, pack_v = lax.fori_loop(0, L, pack0, (zero, zero), unroll=8)
    ys0[0] = pack
    ys0[1] = pack_v
    for n in range(3, 6):
        loads[n].wait()

    pl.semaphore_wait(barrier, len(everyone))
    first = [
        remote(xs0.at[0], xr0.at[1], x_lo),
        remote(xs0.at[1], xr0.at[0], x_hi),
        remote(ys0, yr0.at[1], y_lo),
        remote(ys0, yr0.at[0], y_hi),
        remote(cs.at[0], cup, peers[-1]),
    ]
    for copy in first:
        copy.start()

    cs[L] = zero
    height = ks[...] - g * L
    lid_here = jnp.where(g == groups - 1, ls[...].astype(jnp.float32), 0.0)
    start = jnp.where(g == 0, 1.0, 0.0).astype(jnp.float32)

    def factor(k, held):
        rate, z = held
        here = cs[k]
        above = cs[k + 1]
        keep = height <= k
        delta = 1.0 + here * rate + jnp.where(k == L - 1, lid_here * here, 0.0)
        one = 1.0 / (delta + above)
        rate = jnp.where(keep, delta * one, 1.0)
        one = jnp.where(keep, one, 0.0)
        a = here * one
        z = jnp.where(k == 0, one, a * z)
        im[k] = one
        am[k] = a
        gm[k] = above * one
        gf[k] = z
        return rate, z

    lax.fori_loop(0, L, factor, (zero + start, zero), unroll=4)

    def respond(n, held):
        a, b = held
        k = L - 1 - n
        up = gm[k]
        a = gf[k] + up * a
        b = jnp.where(n == 0, im[L - 1], up * b)
        gf[k] = a
        gl[k] = b
        return a, b

    lax.fori_loop(0, L, respond, (zero, zero), unroll=4)
    own_inv = 1.0 / cs[0]
    sta[g, 0] = gf[0] + own_inv
    sta[g, 1] = gf[L - 1]
    sta[g, 2] = gl[L - 1]
    spread = [remote(sta.at[g], sta.at[g], dev) for dev in peers]
    for copy in spread:
        copy.start()
    loads[6].wait()

    below_sign = jnp.where(g == 0, 0.0, -1.0).astype(jnp.float32)
    above_sign = jnp.where(g == groups - 1, 0.0, -1.0).astype(jnp.float32)
    has_below = jnp.where(g == 0, 0.0, 1.0).astype(jnp.float32)
    up_inv = zero
    pending = []

    for step in range(SUBSTEPS):
        if step == 0:
            for copy in first:
                copy.wait_recv()
            for r in range(2):
                rows_in(ps, r - 2, xr0, 0, r)
                rows_in(ps, I + r, xr0, 1, r)
            rows_in(us, -1, xr0, 0, 2)
            rows_in(us, I, xr0, 1, 2)
            from_lo, from_hi = yr0[0, 0], yr0[1, 0]
            side_lo, side_hi = yr0[0, 1] - pack_v, yr0[1, 1] - pack_v
            spin = jnp.where(sub == 1, pltpu.roll(side_hi, J - 1, 1),
                             jnp.where(sub == 2, -pltpu.roll(side_lo, 1, 1), 0.0))
            up_inv = 1.0 / cup[...]
        else:
            for copy in halo:
                copy.wait_recv()
            n = step - 1
            for r in range(2):
                rows_in(ps, r - 2, xr.at[n], 0, r)
                rows_in(ps, I + r, xr.at[n], 1, r)
            from_lo, from_hi = yr[n, 0], yr[n, 1]
        from_lo = from_lo - pack
        from_hi = from_hi - pack
        mend2 = 0.0625 * jnp.where(sub < 2, pltpu.roll(from_hi, J - 2, 1), pltpu.roll(from_lo, 2, 1))
        mend1 = jnp.where(sub == 1, pltpu.roll(from_hi, J - 1, 1),
                          jnp.where(sub == 2, -pltpu.roll(from_lo, 1, 1), 0.0))
        if step == 0:
            mend2 = mend2 - 0.25 * spin

        def predict(k, _):
            here = ps[k, inner, :]
            fix = jnp.where(edge, pltpu.roll(mend2, J - 2 - 4 * k, 1), 0.0)
            lap = (ps[k, pl.ds(PAD + 2, I), :] + ps[k, pl.ds(PAD - 2, I), :]
                   + pltpu.roll(here, J - 2, 1) + pltpu.roll(here, 2, 1) - 4.0 * here)
            force = 0.0625 * lap + fix
            if step == 0:
                v = vs[k]
                spr = (us[k, pl.ds(PAD + 1, I), :] - us[k, pl.ds(PAD - 1, I), :]
                       + pltpu.roll(v, J - 1, 1) - pltpu.roll(v, 1, 1))
                force = force - 0.25 * spr
            else:
                force = force + fs[k]
            fs[k] = force
            pp[k + 1] = here + force
            return 0

        lax.fori_loop(0, L, predict, 0, unroll=4)
        low = pp[1]
        top = pp[L]
        pp[0] = below_sign * low
        pp[L + 1] = above_sign * top

        def forward(k, z):
            one = im[k]
            z = (ws[k] - 0.5 * (pp[k + 2] - pp[k])) * one + am[k] * z
            zz[k] = z
            return z

        lax.fori_loop(0, L, forward, zero, unroll=4)

        def backward(n, y):
            k = L - 1 - n
            y = zz[k] + gm[k] * y
            zz[k] = y
            return y

        lax.fori_loop(0, L, backward, zero, unroll=4)
        lev[step, g, 0] = zz[0] - 0.5 * low * own_inv
        lev[step, g, 1] = zz[L - 1] + 0.5 * top * up_inv
        pls[step] = top
        around = [remote(lev.at[step, g], lev.at[step, g], dev) for dev in peers]
        around.append(remote(pls.at[step], plr.at[step], peers[0]))
        for copy in around:
            copy.start()

        def move(k, _):
            here = ps[k, inner, :]
            fix = jnp.where(edge, pltpu.roll(mend1, J - 2 - 4 * k, 1), 0.0)
            us[k, inner, :] = us[k, inner, :] - 0.25 * (
                ps[k, pl.ds(PAD + 1, I), :] - ps[k, pl.ds(PAD - 1, I), :])
            vs[k] = vs[k] - 0.25 * (
                pltpu.roll(here, J - 1, 1) - pltpu.roll(here, 1, 1) + fix)
            return 0

        lax.fori_loop(0, L, move, 0, unroll=4)
        if step == SUBSTEPS - 1:
            stores = [
                pltpu.make_async_copy(us.at[:, inner, :], out_u, store_sem.at[0]),
                pltpu.make_async_copy(vs, out_v, store_sem.at[1]),
            ]
            for copy in stores:
                copy.start()

        if step == 0:
            for copy in spread:
                copy.wait_recv()
            d1 = sta[1, 0] + sta[0, 2]
            d2 = sta[2, 0] + sta[1, 2]
            d3 = sta[3, 0] + sta[2, 2]
            q1 = sta[1, 1]
            q2 = sta[2, 1]
            m1 = d2 * d3 - q2 * q2
            whole = 1.0 / (d1 * m1 - q1 * q1 * d3)
            n11 = m1 * whole
            n12 = q1 * d3 * whole
            n13 = q1 * q2 * whole
            n22 = d1 * d3 * whole
            n23 = d1 * q2 * whole
            n33 = (d1 * d2 - q1 * q1) * whole
            for slot, face in ((0, g), (1, g + 1)):
                for col, three in enumerate(((n11, n12, n13), (n12, n22, n23), (n13, n23, n33))):
                    inv[slot, col] = jnp.where(face == 1, three[0], jnp.where(
                        face == 2, three[1], jnp.where(face == 3, three[2], 0.0)))

        for copy in around:
            copy.wait_recv()
        r1 = lev[step, 1, 0] - lev[step, 0, 1]
        r2 = lev[step, 2, 0] - lev[step, 1, 1]
        r3 = lev[step, 3, 0] - lev[step, 2, 1]
        under = inv[0, 0] * r1 + inv[0, 1] * r2 + inv[0, 2] * r3
        over = inv[1, 0] * r1 + inv[1, 1] * r2 + inv[1, 2] * r3
        jump = (under + 0.5 * (low + plr[step])) * own_inv

        def correct(k, held):
            before, acc = held
            x = zz[k] - gf[k] * under + gl[k] * over
            before = jnp.where(k == 0, has_below * (x - jump), before)
            new = pp[k + 1] - 0.5 * (x - before)
            ws[k] = x
            ps[k, inner, :] = new
            if step < SUBSTEPS - 1:
                acc = jnp.where(quad == k, pltpu.roll(new, 4 * k + 2, 1), acc)
            return x, acc

        unused, pack = lax.fori_loop(0, L, correct, (zero, zero), unroll=4)
        pending += around
        if step < SUBSTEPS - 1:
            for r in range(2):
                rows_out(ps, xs.at[step], 0, r, r)
                rows_out(ps, xs.at[step], 1, r, I - 2 + r)
            ys[step] = pack
            halo = [
                remote(xs.at[step, 0], xr.at[step, 1], x_lo),
                remote(xs.at[step, 1], xr.at[step, 0], x_hi),
                remote(ys.at[step], yr.at[step, 1], y_lo),
                remote(ys.at[step], yr.at[step, 0], y_hi),
            ]
            for copy in halo:
                copy.start()
            pending += halo

    stores += [
        pltpu.make_async_copy(ws, out_w, store_sem.at[2]),
        pltpu.make_async_copy(ps.at[:, inner, :], out_p, store_sem.at[3]),
    ]
    for copy in stores[2:]:
        copy.start()
    for copy in first + spread + pending:
        copy.wait_send()
    for copy in stores:
        copy.wait()


def body(zonal, meridional, vertical, pressure, coupling, surface, lid_flag):
    L, I, J = zonal.shape
    IP = I + 2 * PAD
    f32 = jnp.float32
    V = lambda *shape: pltpu.VMEM(shape, f32)
    n_sem = 5 + 3 + 4 * SUBSTEPS + 4 * (SUBSTEPS - 1)
    any_spec = pl.BlockSpec(memory_space=pl.ANY)
    field = jax.ShapeDtypeStruct((L, I, J), f32)
    S = SUBSTEPS
    return tuple(pl.pallas_call(
        kernel,
        out_shape=(field,) * 4,
        in_specs=[any_spec] * 7,
        out_specs=(any_spec,) * 4,
        scratch_shapes=[
            V(L, IP, J), V(L, I, J), V(L, I, J), V(L, IP, J), V(L + 1, I, J),
            pltpu.VMEM((I, J), jnp.int32), pltpu.VMEM((I, J), jnp.int32),
            V(L, I, J), V(L + 2, I, J), V(L, I, J), V(L, I, J), V(L, I, J), V(L, I, J),
            V(L, I, J), V(L, I, J),
            V(2, 3 * L, J), V(2, I, J), V(S - 1, 2, 2 * L, J), V(S - 1, I, J),
            V(2, 3 * L, J), V(2, 2, I, J), V(S - 1, 2, 2 * L, J), V(S - 1, 2, I, J),
            V(4, 3, I, J), V(S, 4, 2, I, J), V(I, J), V(S, I, J), V(S, I, J), V(2, 3, I, J),
            pltpu.SemaphoreType.DMA((7,)),
            pltpu.SemaphoreType.DMA((4,)),
            pltpu.SemaphoreType.DMA((n_sem,)),
            pltpu.SemaphoreType.DMA((n_sem,)),
        ],
        compiler_params=pltpu.CompilerParams(collective_id=0, has_side_effects=True),
    )(zonal, meridional, vertical, pressure, coupling, surface, lid_flag))


def solution(mesh):
    field = P("lev", "gx", "gy")
    plane = P("gx", "gy")
    return jax.shard_map(
        body, mesh=mesh,
        in_specs=(field,) * 5 + (plane,) * 2,
        out_specs=(field,) * 4,
        check_vma=False,
    )
```

```python
import functools

import jax
import jax.numpy as jnp
from jax import lax
from jax.experimental import pallas as pl
from jax.experimental.pallas import tpu as pltpu
from jax.sharding import PartitionSpec as P

SUBSTEPS = 3
MESH = pl.DeviceIdType.MESH
PAD = 8


def kernel(
    zon, mer, ver, pre, cou, sur, lid,
    out_u, out_v, out_w, out_p,
    us, vs, ws, ps, cs, ks, ls,
    fs, pp, zz, am, im, gm, gf, gl,
    xs0, ys0, xs, ys, xr0, yr0, xr, yr,
    sta, lev, cup, pls, plr, inv,
    load_sem, send_sem, recv_sem,
):
    L, I, J = zon.shape
    g = lax.axis_index("lev")
    gx = lax.axis_index("gx")
    gy = lax.axis_index("gy")
    groups = lax.axis_size("lev")
    nx = lax.axis_size("gx")
    ny = lax.axis_size("gy")
    x_lo = {"gx": lax.rem(gx + nx - 1, nx)}
    x_hi = {"gx": lax.rem(gx + 1, nx)}
    y_lo = {"gy": lax.rem(gy + ny - 1, ny)}
    y_hi = {"gy": lax.rem(gy + 1, ny)}
    peers = [{"lev": lax.rem(g + d, groups)} for d in range(1, groups)]
    inner = pl.ds(PAD, I)

    loads = [
        pltpu.make_async_copy(src, dst, load_sem.at[n])
        for n, (src, dst) in enumerate([
            (pre, ps.at[:, inner, :]),
            (mer, vs),
            (zon, us.at[:, inner, :]),
            (cou, cs.at[pl.ds(0, L)]),
            (sur, ks),
            (lid, ls),
            (ver, ws),
        ])
    ]
    for copy in loads:
        copy.start()
    barrier = pltpu.get_barrier_semaphore()
    everyone = [x_lo, x_hi, y_lo, y_hi] + peers
    for dev in everyone:
        pl.semaphore_signal(barrier, inc=1, device_id=dev, device_id_type=MESH)

    lane = lax.broadcasted_iota(jnp.int32, (I, J), 1)
    quad = lane // 4
    sub = lane % 4
    edge = (lane < 2) | (lane >= J - 2)
    zero = jnp.zeros((I, J), jnp.float32)

    def rows_out(src2, buf, side, at, row):
        buf[side, pl.ds(at * L, L), :] = src2[:, PAD + row, :]

    def rows_in(dst2, row, buf, side, at):
        dst2[:, PAD + row, :] = buf[side, pl.ds(at * L, L), :]

    sems = iter(range(64))

    def remote(src, dst, dev):
        n = next(sems)
        return pltpu.make_async_remote_copy(
            src_ref=src, dst_ref=dst, send_sem=send_sem.at[n], recv_sem=recv_sem.at[n],
            device_id=dev, device_id_type=MESH)

    loads[0].wait()
    loads[1].wait()
    loads[2].wait()
    for r in range(2):
        rows_out(ps, xs0, 0, r, r)
        rows_out(ps, xs0, 1, r, I - 2 + r)
    rows_out(us, xs0, 0, 2, 0)
    rows_out(us, xs0, 1, 2, I - 1)

    def pack0(k, held):
        a, b = held
        turn = 4 * k + 2
        mine = quad == k
        a = jnp.where(mine, pltpu.roll(ps[k, inner, :], turn, 1), a)
        b = jnp.where(mine, pltpu.roll(vs[k], turn, 1), b)
        return a, b

    pack, pack_v = lax.fori_loop(0, L, pack0, (zero, zero), unroll=8)
    ys0[0] = pack
    ys0[1] = pack_v
    for n in range(3, 6):
        loads[n].wait()

    pl.semaphore_wait(barrier, len(everyone))
    first = [
        remote(xs0.at[0], xr0.at[1], x_lo),
        remote(xs0.at[1], xr0.at[0], x_hi),
        remote(ys0, yr0.at[1], y_lo),
        remote(ys0, yr0.at[0], y_hi),
        remote(cs.at[0], cup, peers[-1]),
    ]
    for copy in first:
        copy.start()

    cs[L] = zero
    height = ks[...] - g * L
    lid_here = jnp.where(g == groups - 1, ls[...].astype(jnp.float32), 0.0)
    start = jnp.where(g == 0, 1.0, 0.0).astype(jnp.float32)

    def factor(k, held):
        rate, z = held
        here = cs[k]
        above = cs[k + 1]
        keep = height <= k
        delta = 1.0 + here * rate + jnp.where(k == L - 1, lid_here * here, 0.0)
        one = 1.0 / (delta + above)
        rate = jnp.where(keep, delta * one, 1.0)
        one = jnp.where(keep, one, 0.0)
        a = here * one
        z = jnp.where(k == 0, one, a * z)
        im[k] = one
        am[k] = a
        gm[k] = above * one
        gf[k] = z
        return rate, z

    lax.fori_loop(0, L, factor, (zero + start, zero), unroll=4)

    def respond(n, held):
        a, b = held
        k = L - 1 - n
        up = gm[k]
        a = gf[k] + up * a
        b = jnp.where(n == 0, im[L - 1], up * b)
        gf[k] = a
        gl[k] = b
        return a, b

    lax.fori_loop(0, L, respond, (zero, zero), unroll=4)
    own_inv = 1.0 / cs[0]
    sta[g, 0] = gf[0] + own_inv
    sta[g, 1] = gf[L - 1]
    sta[g, 2] = gl[L - 1]
    spread = [remote(sta.at[g], sta.at[g], dev) for dev in peers]
    for copy in spread:
        copy.start()
    loads[6].wait()

    below_sign = jnp.where(g == 0, 0.0, -1.0).astype(jnp.float32)
    above_sign = jnp.where(g == groups - 1, 0.0, -1.0).astype(jnp.float32)
    has_below = jnp.where(g == 0, 0.0, 1.0).astype(jnp.float32)
    up_inv = zero
    pending = []

    for step in range(SUBSTEPS):
        last = step == SUBSTEPS - 1
        if step == 0:
            for copy in first:
                copy.wait_recv()
            for r in range(2):
                rows_in(ps, r - 2, xr0, 0, r)
                rows_in(ps, I + r, xr0, 1, r)
            rows_in(us, -1, xr0, 0, 2)
            rows_in(us, I, xr0, 1, 2)
            from_lo, from_hi = yr0[0, 0], yr0[1, 0]
            side_lo, side_hi = yr0[0, 1] - pack_v, yr0[1, 1] - pack_v
            spin = jnp.where(sub == 1, pltpu.roll(side_hi, J - 1, 1),
                             jnp.where(sub == 2, -pltpu.roll(side_lo, 1, 1), 0.0))
            up_inv = 1.0 / cup[...]
        else:
            for copy in halo:
                copy.wait_recv()
            n = step - 1
            for r in range(2):
                rows_in(ps, r - 2, xr.at[n], 0, r)
                rows_in(ps, I + r, xr.at[n], 1, r)
            from_lo, from_hi = yr[n, 0], yr[n, 1]
        from_lo = from_lo - pack
        from_hi = from_hi - pack
        mend2 = 0.0625 * jnp.where(sub < 2, pltpu.roll(from_hi, J - 2, 1), pltpu.roll(from_lo, 2, 1))
        mend1 = jnp.where(sub == 1, pltpu.roll(from_hi, J - 1, 1),
                          jnp.where(sub == 2, -pltpu.roll(from_lo, 1, 1), 0.0))
        if step == 0:
            mend2 = mend2 - 0.25 * spin

        def predict(k, _):
            here = ps[k, inner, :]
            fix = jnp.where(edge, pltpu.roll(mend2, J - 2 - 4 * k, 1), 0.0)
            lap = (ps[k, pl.ds(PAD + 2, I), :] + ps[k, pl.ds(PAD - 2, I), :]
                   + pltpu.roll(here, J - 2, 1) + pltpu.roll(here, 2, 1) - 4.0 * here)
            force = 0.0625 * lap + fix
            if step == 0:
                v = vs[k]
                spr = (us[k, pl.ds(PAD + 1, I), :] - us[k, pl.ds(PAD - 1, I), :]
                       + pltpu.roll(v, J - 1, 1) - pltpu.roll(v, 1, 1))
                force = force - 0.25 * spr
            else:
                force = force + fs[k]
            fs[k] = force
            pp[k + 1] = here + force
            return 0

        lax.fori_loop(0, L, predict, 0, unroll=4)
        low = pp[1]
        top = pp[L]
        pp[0] = below_sign * low
        pp[L + 1] = above_sign * top

        def forward(k, z):
            one = im[k]
            z = (ws[k] - 0.5 * (pp[k + 2] - pp[k])) * one + am[k] * z
            zz[k] = z
            return z

        lax.fori_loop(0, L, forward, zero, unroll=4)

        def backward(n, y):
            k = L - 1 - n
            y = zz[k] + gm[k] * y
            zz[k] = y
            return y

        lax.fori_loop(0, L, backward, zero, unroll=4)
        lev[step, g, 0] = zz[0] - 0.5 * low * own_inv
        lev[step, g, 1] = zz[L - 1] + 0.5 * top * up_inv
        pls[step] = top
        around = [remote(lev.at[step, g], lev.at[step, g], dev) for dev in peers]
        around.append(remote(pls.at[step], plr.at[step], peers[0]))
        for copy in around:
            copy.start()

        def move(k, _):
            here = ps[k, inner, :]
            fix = jnp.where(edge, pltpu.roll(mend1, J - 2 - 4 * k, 1), 0.0)
            new_u = us[k, inner, :] - 0.25 * (
                ps[k, pl.ds(PAD + 1, I), :] - ps[k, pl.ds(PAD - 1, I), :])
            new_v = vs[k] - 0.25 * (
                pltpu.roll(here, J - 1, 1) - pltpu.roll(here, 1, 1) + fix)
            if last:
                out_u[k] = new_u
                out_v[k] = new_v
            else:
                us[k, inner, :] = new_u
                vs[k] = new_v
            return 0

        lax.fori_loop(0, L, move, 0, unroll=4)
        if step == 0:
            for copy in spread:
                copy.wait_recv()
            d1 = sta[1, 0] + sta[0, 2]
            d2 = sta[2, 0] + sta[1, 2]
            d3 = sta[3, 0] + sta[2, 2]
            q1 = sta[1, 1]
            q2 = sta[2, 1]
            m1 = d2 * d3 - q2 * q2
            whole = 1.0 / (d1 * m1 - q1 * q1 * d3)
            n11 = m1 * whole
            n12 = q1 * d3 * whole
            n13 = q1 * q2 * whole
            n22 = d1 * d3 * whole
            n23 = d1 * q2 * whole
            n33 = (d1 * d2 - q1 * q1) * whole
            for slot, face in ((0, g), (1, g + 1)):
                for col, three in enumerate(((n11, n12, n13), (n12, n22, n23), (n13, n23, n33))):
                    inv[slot, col] = jnp.where(face == 1, three[0], jnp.where(
                        face == 2, three[1], jnp.where(face == 3, three[2], 0.0)))

        for copy in around:
            copy.wait_recv()
        r1 = lev[step, 1, 0] - lev[step, 0, 1]
        r2 = lev[step, 2, 0] - lev[step, 1, 1]
        r3 = lev[step, 3, 0] - lev[step, 2, 1]
        under = inv[0, 0] * r1 + inv[0, 1] * r2 + inv[0, 2] * r3
        over = inv[1, 0] * r1 + inv[1, 1] * r2 + inv[1, 2] * r3
        jump = (under + 0.5 * (low + plr[step])) * own_inv

        def correct(k, held):
            before, acc = held
            x = zz[k] - gf[k] * under + gl[k] * over
            before = jnp.where(k == 0, has_below * (x - jump), before)
            new = pp[k + 1] - 0.5 * (x - before)
            if last:
                out_w[k] = x
                out_p[k] = new
            else:
                ws[k] = x
                ps[k, inner, :] = new
                acc = jnp.where(quad == k, pltpu.roll(new, 4 * k + 2, 1), acc)
            return x, acc

        unused, pack = lax.fori_loop(0, L, correct, (zero, zero), unroll=4)
        pending += around
        if not last:
            for r in range(2):
                rows_out(ps, xs.at[step], 0, r, r)
                rows_out(ps, xs.at[step], 1, r, I - 2 + r)
            ys[step] = pack
            halo = [
                remote(xs.at[step, 0], xr.at[step, 1], x_lo),
                remote(xs.at[step, 1], xr.at[step, 0], x_hi),
                remote(ys.at[step], yr.at[step, 1], y_lo),
                remote(ys.at[step], yr.at[step, 0], y_hi),
            ]
            for copy in halo:
                copy.start()
            pending += halo

    for copy in first + spread + pending:
        copy.wait_send()


def store_kernel(*refs):
    sem = refs[-1]
    copies = [
        pltpu.make_async_copy(refs[n], refs[4 + n], sem.at[n]) for n in range(4)
    ]
    for copy in copies:
        copy.start()
    for copy in copies:
        copy.wait()


def body(zonal, meridional, vertical, pressure, coupling, surface, lid_flag):
    L, I, J = zonal.shape
    IP = I + 2 * PAD
    f32 = jnp.float32
    V = lambda *shape: pltpu.VMEM(shape, f32)
    n_sem = 5 + 3 + 4 * SUBSTEPS + 4 * (SUBSTEPS - 1)
    any_spec = pl.BlockSpec(memory_space=pl.ANY)
    field = jax.ShapeDtypeStruct((L, I, J), f32)
    S = SUBSTEPS
    vmem_spec = pl.BlockSpec(memory_space=pltpu.VMEM)
    results = pl.pallas_call(
        kernel,
        out_shape=(V(L, I, J),) * 4,
        in_specs=[any_spec] * 7,
        out_specs=(vmem_spec,) * 4,
        scratch_shapes=[
            V(L, IP, J), V(L, I, J), V(L, I, J), V(L, IP, J), V(L + 1, I, J),
            pltpu.VMEM((I, J), jnp.int32), pltpu.VMEM((I, J), jnp.int32),
            V(L, I, J), V(L + 2, I, J), V(L, I, J), V(L, I, J), V(L, I, J), V(L, I, J),
            V(L, I, J), V(L, I, J),
            V(2, 3 * L, J), V(2, I, J), V(S - 1, 2, 2 * L, J), V(S - 1, I, J),
            V(2, 3 * L, J), V(2, 2, I, J), V(S - 1, 2, 2 * L, J), V(S - 1, 2, I, J),
            V(4, 3, I, J), V(S, 4, 2, I, J), V(I, J), V(S, I, J), V(S, I, J), V(2, 3, I, J),
            pltpu.SemaphoreType.DMA((7,)),
            pltpu.SemaphoreType.DMA((n_sem,)),
            pltpu.SemaphoreType.DMA((n_sem,)),
        ],
        compiler_params=pltpu.CompilerParams(collective_id=0, has_side_effects=True),
    )(zonal, meridional, vertical, pressure, coupling, surface, lid_flag)
    return tuple(pl.pallas_call(
        store_kernel,
        out_shape=(field,) * 4,
        in_specs=[vmem_spec] * 4,
        out_specs=(any_spec,) * 4,
        scratch_shapes=[pltpu.SemaphoreType.DMA((4,))],
        compiler_params=pltpu.CompilerParams(vmem_limit_bytes=1 << 22),
    )(*results))


def solution(mesh):
    field = P("lev", "gx", "gy")
    plane = P("gx", "gy")
    return jax.shard_map(
        body, mesh=mesh,
        in_specs=(field,) * 5 + (plane,) * 2,
        out_specs=(field,) * 4,
        check_vma=False,
    )
```

```python
import functools
import types

import jax
import jax.numpy as jnp
from jax import lax
from jax.experimental import pallas as pl
from jax.experimental.pallas import tpu as pltpu
from jax.sharding import PartitionSpec as P

SUBSTEPS = 3
MESH = pl.DeviceIdType.MESH
PAD = 8
GROUPS = 4


def inverse(d1, d2, d3, q1, q2):
    m1 = d2 * d3 - q2 * q2
    whole = 1.0 / (d1 * m1 - q1 * q1 * d3)
    n12 = q1 * d3 * whole
    n13 = q1 * q2 * whole
    n23 = d1 * q2 * whole
    return (
        (m1 * whole, n12, n13),
        (n12, d1 * d3 * whole, n23),
        (n13, n23, (d1 * d2 - q1 * q1) * whole),
    )


def face_row(rows, col, face):
    return jnp.where(face == 1, rows[0][col], jnp.where(
        face == 2, rows[1][col], jnp.where(face == 3, rows[2][col], 0.0)))


def kernel(names, zon, mer, ver, pre, cou, sur, lid, out_u, out_v, out_w, out_p, *scratch):
    m = types.SimpleNamespace(**dict(zip(names, scratch)))
    us, vs, ws, ps, cs = m.us, m.vs, m.ws, m.ps, m.cs
    L, I, J = zon.shape
    g = lax.axis_index("lev")
    gx = lax.axis_index("gx")
    gy = lax.axis_index("gy")
    nx = lax.axis_size("gx")
    ny = lax.axis_size("gy")
    groups = GROUPS
    x_dev = ({"gx": lax.rem(gx + nx - 1, nx)}, {"gx": lax.rem(gx + 1, nx)})
    y_dev = ({"gy": lax.rem(gy + ny - 1, ny)}, {"gy": lax.rem(gy + 1, ny)})
    peers = [{"lev": lax.rem(g + d, groups)} for d in range(1, groups)]
    around = [{**dev, "lev": lax.rem(g + d, groups)}
              for d in range(groups) for dev in x_dev + y_dev]
    inner = pl.ds(PAD, I)

    loads = [
        pltpu.make_async_copy(src, dst, m.load_sem.at[n])
        for n, (src, dst) in enumerate([
            (pre, ps.at[:, inner, :]),
            (mer, vs),
            (zon, us.at[:, inner, :]),
            (cou, cs.at[pl.ds(0, L)]),
            (sur, m.ks),
            (lid, m.ls),
            (ver, ws),
        ])
    ]
    for copy in loads:
        copy.start()
    barrier = pltpu.get_barrier_semaphore()
    everyone = peers + around
    for dev in everyone:
        pl.semaphore_signal(barrier, inc=1, device_id=dev, device_id_type=MESH)

    lane = lax.broadcasted_iota(jnp.int32, (I, J), 1)
    level = lax.broadcasted_iota(jnp.int32, (L, J), 0)
    quad = lane // 4
    sub = lane % 4
    edge = (lane < 2) | (lane >= J - 2)
    lane8 = lax.broadcasted_iota(jnp.int32, (8, J), 1)
    quad8 = lane8 // 4
    left8 = lane8 % 4 < 2
    live8 = (quad8 % 4 == 0) & (quad8 < 16)
    zero = jnp.zeros((I, J), jnp.float32)
    halo_rows = jnp.zeros((L, PAD, J), jnp.float32)
    for ref in (ps, us):
        ref[:, 0:PAD, :] = halo_rows
        ref[:, PAD + I:, :] = halo_rows
    pick = lax.broadcasted_iota(jnp.int32, (J, 4 * J), 0)
    into = lax.broadcasted_iota(jnp.int32, (J, 4 * J), 1)
    m.sel[...] = jnp.where(
        (pick % 16 == into % 4) & (pick // 16 == into // J), 1.0, 0.0).astype(jnp.float32)

    counter = iter(range(1 << 10))

    def remote(src, dst, dev):
        n = next(counter)
        return pltpu.make_async_remote_copy(
            src_ref=src, dst_ref=dst, send_sem=m.send_sem.at[n], recv_sem=m.recv_sem.at[n],
            device_id=dev, device_id_type=MESH)

    sent = []

    def start(copies):
        for copy in copies:
            copy.start()
        sent.extend(copies)
        return copies

    def arrive(copies):
        for copy in copies:
            copy.wait_recv()

    def side_row(side, r):
        return r if side == 0 else I - 2 + r

    def packed(k, plane, held):
        return jnp.where(quad == k, pltpu.roll(plane, 4 * k + 2, 1), held)

    def strips(phase, planes):
        tile = jnp.zeros((8, J), jnp.float32)
        for n, plane in enumerate(planes):
            m.xsi[phase, 0, pl.ds(2 * n, 2), :] = plane[0:2]
            m.xsi[phase, 1, pl.ds(2 * n, 2), :] = plane[I - 2:I]
            for v in range(4):
                turned = pltpu.roll(plane[8 * v:8 * v + 8], 16 * v + 4 * n + 2, 1)
                tile = jnp.where(quad8 == 4 * v + n, turned, tile)
        m.ysi[phase] = tile
        return start([
            copy
            for d in range(groups) for side in range(2)
            for copy in (
                remote(m.xsi.at[phase, side], m.xri.at[phase, 1 - side, g], around[4 * d + side]),
                remote(m.ysi.at[phase], m.yri.at[phase, 1 - side, g], around[4 * d + 2 + side]),
            )
        ])

    def x_rows(phase, side, h, n):
        return m.xri[phase, side, h, pl.ds(2 * n, 2), :]

    def y_tile(phase, h):
        return jnp.where(left8, m.yri[phase, 0, h], m.yri[phase, 1, h])

    def turn8(tile, n):
        return pltpu.roll(tile, J - 4 * n, 1) if n else tile

    loads[0].wait()
    loads[1].wait()
    loads[2].wait()
    for side in range(2):
        for r in range(2):
            m.xs0[side, pl.ds(r * L, L), :] = ps[:, PAD + side_row(side, r), :]
        m.xs0[side, pl.ds(2 * L, L), :] = us[:, PAD + (I - 1) * side, :]

    def pack0(k, held):
        return packed(k, ps[k, inner, :], held[0]), packed(k, vs[k], held[1])

    pack, pack_v = lax.fori_loop(0, L, pack0, (zero, zero), unroll=16)
    m.ys0[0] = pack
    m.ys0[1] = pack_v
    for n in range(3, 6):
        loads[n].wait()

    pl.semaphore_wait(barrier, len(everyone))
    first = start([
        remote(m.xs0.at[0], m.xr0.at[1], x_dev[0]),
        remote(m.xs0.at[1], m.xr0.at[0], x_dev[1]),
        remote(m.ys0, m.yr0.at[1], y_dev[0]),
        remote(m.ys0, m.yr0.at[0], y_dev[1]),
        remote(cs.at[0], m.cup, peers[-1]),
    ])

    cs[L] = zero
    height = m.ks[...] - g * L
    lid_here = jnp.where(g == groups - 1, m.ls[...].astype(jnp.float32), 0.0)
    is_first = jnp.where(g == 0, 1.0, 0.0).astype(jnp.float32)
    above_sign = jnp.where(g == groups - 1, 0.0, -1.0).astype(jnp.float32)
    g_below = lax.rem(g + groups - 1, groups)

    def factor(k, held):
        rate, z = held
        here = cs[k]
        above = cs[k + 1]
        keep = height <= k
        delta = 1.0 + here * rate + jnp.where(k == L - 1, lid_here * here, 0.0)
        one = 1.0 / (delta + above)
        rate = jnp.where(keep, delta * one, 1.0)
        one = jnp.where(keep, one, 0.0)
        a = here * one
        z = jnp.where(k == 0, one, a * z)
        m.im[k] = one
        m.am[k] = a
        m.gm[k] = above * one
        m.gf[k] = z
        return rate, z

    lax.fori_loop(0, L, factor, (zero + is_first, zero), unroll=4)

    def respond(n, held):
        a, b = held
        k = L - 1 - n
        up = m.gm[k]
        a = m.gf[k] + up * a
        b = jnp.where(n == 0, m.im[L - 1], up * b)
        m.gf[k] = a
        m.gl[k] = b
        return a, b

    lax.fori_loop(0, L, respond, (zero, zero), unroll=4)
    own_inv = 1.0 / cs[0]
    own_static = (m.gf[0] + own_inv, m.gf[L - 1], m.gl[L - 1])
    for n in range(3):
        m.sta[g, n] = own_static[n]
    static = start([remote(m.sta.at[g], m.sta.at[g], dev) for dev in peers])
    spare = jnp.zeros((2, J), jnp.float32)
    for phase in range(SUBSTEPS):
        for side in range(2):
            m.xsi[phase, side, pl.ds(6, 2), :] = spare
    static += strips(0, own_static)

    def slopes(k, held):
        f_before, l_before, a_pack, b_pack = held
        f = m.gf[k]
        l = m.gl[k]
        a = jnp.where(k == 0, (is_first - 1.0) * 0.5 * own_inv, 0.5 * (f - f_before))
        b = jnp.where(k == 0, is_first * -0.5 * l, -0.5 * (l - l_before))
        m.aa[k] = a
        m.bb[k] = b
        return f, l, packed(k, a, a_pack), packed(k, b, b_pack)

    unused_f, unused_l, a_pack, b_pack = lax.fori_loop(0, L, slopes, (zero,) * 4, unroll=8)
    m.ysa[0] = a_pack
    m.ysa[1] = b_pack
    for side in range(2):
        for r in range(2):
            m.xsa[side, pl.ds(r * L, L), :] = m.aa[:, side_row(side, r), :]
            m.xsa[side, pl.ds((2 + r) * L, L), :] = m.bb[:, side_row(side, r), :]
    static += start([
        remote(m.xsa.at[0], m.xra.at[1], x_dev[0]),
        remote(m.xsa.at[1], m.xra.at[0], x_dev[1]),
        remote(m.ysa, m.yra.at[1], y_dev[0]),
        remote(m.ysa, m.yra.at[0], y_dev[1]),
    ])

    def predict(step, k, _):
        here = ps[k, inner, :]
        force = 0.0625 * (
            ps[k, pl.ds(PAD + 2, I), :] + ps[k, pl.ds(PAD - 2, I), :]
            + pltpu.roll(here, J - 2, 1) + pltpu.roll(here, 2, 1) - 4.0 * here)
        if step == 0:
            v = vs[k]
            force = force - 0.25 * (
                us[k, pl.ds(PAD + 1, I), :] - us[k, pl.ds(PAD - 1, I), :]
                + pltpu.roll(v, J - 1, 1) - pltpu.roll(v, 1, 1))
        else:
            force = force + m.fs[k]
        m.fs[k] = force
        m.pp[k + 1] = here + force
        return 0

    lax.fori_loop(0, L, functools.partial(predict, 0), 0, unroll=16)
    loads[6].wait()

    up_inv = zero
    messages = first
    for step in range(SUBSTEPS):
        last = step == SUBSTEPS - 1
        arrive(messages)
        rows = []
        if step == 0:
            for side in range(2):
                rows += [m.xr0[side, pl.ds(r * L, L), :] for r in range(2)]
            diff = jnp.where(sub < 2, m.yr0[0, 0], m.yr0[1, 0]) - pack
            drift = jnp.where(sub < 2, m.yr0[0, 1], m.yr0[1, 1]) - pack_v
            spin = jnp.where(sub == 1, pltpu.roll(drift, J - 1, 1),
                             jnp.where(sub == 2, -pltpu.roll(drift, 1, 1), 0.0))
            up_inv = 1.0 / m.cup[...]
        else:
            for side in range(2):
                jumps = [x_rows(step, side, h, 0) - x_rows(step, side, h - 1, 1) for h in (1, 2, 3)]
                lower = sum(m.nx[side, n, 0:2, :] * jumps[n] for n in range(3))
                upper = sum(m.nx[side, 3 + n, 0:2, :] * jumps[n] for n in range(3))
                floor = lower + 0.5 * x_rows(step, side, g_below, 2)
                for r in range(2):
                    low_r = jnp.where(level == 0, floor[r:r + 1], lower[r:r + 1])
                    rows.append(
                        m.xr[step - 1, side, pl.ds(r * L, L), :]
                        + m.xra[side, pl.ds(r * L, L), :] * low_r
                        + m.xra[side, pl.ds((2 + r) * L, L), :] * upper[r:r + 1])
            tiles = [y_tile(step, h) for h in range(groups)]
            jumps = [tiles[h] - turn8(tiles[h - 1], 1) for h in (1, 2, 3)]
            lower = sum(m.ny[n] * jumps[n] for n in range(3))
            upper = sum(m.ny[3 + n] * jumps[n] for n in range(3))
            floor = jnp.where(live8, lower + 0.5 * turn8(y_tile(step, g_below), 2), 0.0)
            wide = jnp.dot(jnp.concatenate([lower, upper, floor], 0), m.sel[...],
                           preferred_element_type=jnp.float32, precision=lax.Precision.HIGHEST)
            parts = [jnp.concatenate([wide[8 * n:8 * n + 8, J * v:J * v + J] for v in range(4)], 0)
                     for n in range(3)]
            diff = (jnp.where(sub < 2, m.yr[step - 1, 0], m.yr[step - 1, 1])
                    + m.am2[...] * jnp.where(quad == 0, parts[2], parts[0])
                    + m.bm2[...] * parts[1]) - pack
        mend2 = 0.0625 * jnp.where(sub < 2, pltpu.roll(diff, J - 2, 1), pltpu.roll(diff, 2, 1))
        mend1 = jnp.where(sub == 1, pltpu.roll(diff, J - 1, 1),
                          jnp.where(sub == 2, -pltpu.roll(diff, 1, 1), 0.0))
        adds = [0.0625 * row for row in rows]
        if step == 0:
            mend2 = mend2 - 0.25 * spin
            adds[0] = adds[0] + 0.25 * m.xr0[0, pl.ds(2 * L, L), :]
            adds[3] = adds[3] - 0.25 * m.xr0[1, pl.ds(2 * L, L), :]
        for at, add in zip((0, 1, I - 2, I - 1), adds):
            m.fs[:, at, :] = m.fs[:, at, :] + add
            m.pp[pl.ds(1, L), at, :] = m.pp[pl.ds(1, L), at, :] + add
        m.hx[0] = rows[1]
        m.hx[1] = rows[2]

        def patch(k, _):
            fix = jnp.where(edge, pltpu.roll(mend2, J - 2 - 4 * k, 1), 0.0)
            m.fs[k] = m.fs[k] + fix
            m.pp[k + 1] = m.pp[k + 1] + fix
            return 0

        lax.fori_loop(0, L, patch, 0, unroll=16)

        low = m.pp[1]
        top = m.pp[L]
        m.pp[0] = (is_first - 1.0) * low
        m.pp[L + 1] = above_sign * top
        m.pls[step] = top
        row_up = start([remote(m.pls.at[step], m.plr.at[step], peers[0])])

        def forward(k, z):
            z = (ws[k] - 0.5 * (m.pp[k + 2] - m.pp[k])) * m.im[k] + m.am[k] * z
            m.zz[k] = z
            return z

        lax.fori_loop(0, L, forward, zero, unroll=8)

        def backward(n, y):
            k = L - 1 - n
            y = m.zz[k] + m.gm[k] * y
            m.zz[k] = y
            return y

        y_low = lax.fori_loop(0, L, backward, zero, unroll=8)
        down = y_low - 0.5 * low * own_inv
        up = m.zz[L - 1] + 0.5 * top * up_inv
        m.lev[step, g, 0] = down
        m.lev[step, g, 1] = up
        group_rows = start([remote(m.lev.at[step, g], m.lev.at[step, g], dev) for dev in peers])
        if not last:
            messages = strips(step + 1, (down, up, top))

        def plain(k, held):
            before, acc = held
            y = m.zz[k]
            q = m.pp[k + 1] - 0.5 * (y - before)
            m.qs[k] = q
            return y, acc if last else packed(k, q, acc)

        ghost = y_low - (is_first * y_low - m.aa[0] * low)
        unused_y, q_pack = lax.fori_loop(0, L, plain, (ghost, zero), unroll=16)
        if not last:
            for side in range(2):
                for r in range(2):
                    m.xs[step, side, pl.ds(r * L, L), :] = m.qs[:, side_row(side, r), :]
            m.ys[step] = q_pack
            messages += start([
                remote(m.xs.at[step, 0], m.xr.at[step, 1], x_dev[0]),
                remote(m.xs.at[step, 1], m.xr.at[step, 0], x_dev[1]),
                remote(m.ys.at[step], m.yr.at[step, 1], y_dev[0]),
                remote(m.ys.at[step], m.yr.at[step, 0], y_dev[1]),
            ])


        def move(k, _):
            here = ps[k, inner, :]
            fix = jnp.where(edge, pltpu.roll(mend1, J - 2 - 4 * k, 1), 0.0)
            new_u = us[k, inner, :] - 0.25 * (
                ps[k, pl.ds(PAD + 1, I), :] - ps[k, pl.ds(PAD - 1, I), :])
            new_v = vs[k] - 0.25 * (
                pltpu.roll(here, J - 1, 1) - pltpu.roll(here, 1, 1) + fix)
            if last:
                out_u[k] = new_u
                out_v[k] = new_v
            else:
                us[k, inner, :] = new_u
                vs[k] = new_v
            return 0

        lax.fori_loop(0, L, move, 0, unroll=8)
        for end, at in ((0, 0), (1, I - 1)):
            kick = (0.25 - 0.5 * end) * m.hx[end]
            if last:
                out_u[:, at, :] = out_u[:, at, :] + kick
            else:
                us[:, PAD + at, :] = us[:, PAD + at, :] + kick

        if step == 0:
            arrive(static)
            sta = m.sta
            rows_of = inverse(sta[1, 0] + sta[0, 2], sta[2, 0] + sta[1, 2], sta[3, 0] + sta[2, 2],
                              sta[1, 1], sta[2, 1])
            for slot in range(2):
                for col in range(3):
                    m.inv[slot, col] = face_row(rows_of, col, g + slot)
            for side in range(2):
                part = lambda h, n: x_rows(0, side, h, n)
                rows_of = inverse(part(1, 0) + part(0, 2), part(2, 0) + part(1, 2),
                                  part(3, 0) + part(2, 2), part(1, 1), part(2, 1))
                for slot in range(2):
                    for col in range(3):
                        m.nx[side, 3 * slot + col, 0:2, :] = face_row(rows_of, col, g + slot)
            tiles = [y_tile(0, h) for h in range(groups)]
            part = lambda h, n: jnp.where(live8, turn8(tiles[h], n), 1.0)
            rows_of = inverse(part(1, 0) + part(0, 2), part(2, 0) + part(1, 2),
                              part(3, 0) + part(2, 2), part(1, 1), part(2, 1))
            for slot in range(2):
                for col in range(3):
                    m.ny[3 * slot + col] = jnp.where(live8, face_row(rows_of, col, g + slot), 0.0)
            m.am2[...] = jnp.where(sub < 2, m.yra[0, 0], m.yra[1, 0])
            m.bm2[...] = jnp.where(sub < 2, m.yra[0, 1], m.yra[1, 1])

        arrive(group_rows + row_up)
        jumps = [m.lev[step, h, 0] - m.lev[step, h - 1, 1] for h in (1, 2, 3)]
        under = sum(m.inv[0, n] * jumps[n] for n in range(3))
        over = sum(m.inv[1, n] * jumps[n] for n in range(3))
        under0 = under + 0.5 * m.plr[step]

        def correct(k, acc):
            x = m.zz[k] - m.gf[k] * under + m.gl[k] * over
            new = m.qs[k] + m.aa[k] * jnp.where(k == 0, under0, under) + m.bb[k] * over
            if last:
                out_w[k] = x
                out_p[k] = new
                return acc
            ws[k] = x
            ps[k, inner, :] = new
            return packed(k, new, acc)

        pack = lax.fori_loop(0, L, correct, zero, unroll=16)
        if not last:
            lax.fori_loop(0, L, functools.partial(predict, step + 1), 0, unroll=16)

    for copy in sent:
        copy.wait_send()


def store_kernel(*refs):
    sem = refs[-1]
    copies = [
        pltpu.make_async_copy(refs[n], refs[4 + n], sem.at[n]) for n in range(4)
    ]
    for copy in copies:
        copy.start()
    for copy in copies:
        copy.wait()


def body(zonal, meridional, vertical, pressure, coupling, surface, lid_flag):
    L, I, J = zonal.shape
    IP = I + 2 * PAD
    S = SUBSTEPS
    G = GROUPS
    f32 = jnp.float32
    n_sem = 5 + (G - 1) + 4 * G + 4 + S * G + (S - 1) * (4 * G + 4)
    V = lambda *shape: pltpu.VMEM(shape, f32)
    level = (L, I, J)
    scratch = dict(
        us=V(L, IP, J), vs=V(*level), ws=V(*level), ps=V(L, IP, J), cs=V(L + 1, I, J),
        ks=pltpu.VMEM((I, J), jnp.int32), ls=pltpu.VMEM((I, J), jnp.int32),
        fs=V(*level), pp=V(L + 2, I, J), zz=V(*level), qs=V(*level),
        am=V(*level), im=V(*level), gm=V(*level), gf=V(*level), gl=V(*level),
        aa=V(*level), bb=V(*level),
        xs0=V(2, 3 * L, J), ys0=V(2, I, J), xr0=V(2, 3 * L, J), yr0=V(2, 2, I, J),
        xs=V(S - 1, 2, 2 * L, J), ys=V(S - 1, I, J),
        xr=V(S - 1, 2, 2 * L, J), yr=V(S - 1, 2, I, J),
        xsa=V(2, 4 * L, J), ysa=V(2, I, J), xra=V(2, 4 * L, J), yra=V(2, 2, I, J),
        xsi=V(S, 2, 8, J), ysi=V(S, 8, J), xri=V(S, 2, G, 8, J), yri=V(S, 2, G, 8, J),
        sta=V(G, 3, I, J), lev=V(S, G, 2, I, J), cup=V(I, J),
        pls=V(S, I, J), plr=V(S, I, J), hx=V(2, L, J),
        inv=V(2, 3, I, J), nx=V(2, 6, 8, J), ny=V(6, 8, J), am2=V(I, J), bm2=V(I, J),
        sel=V(J, 4 * J),
        load_sem=pltpu.SemaphoreType.DMA((7,)),
        send_sem=pltpu.SemaphoreType.DMA((n_sem,)),
        recv_sem=pltpu.SemaphoreType.DMA((n_sem,)),
    )
    any_spec = pl.BlockSpec(memory_space=pl.ANY)
    vmem_spec = pl.BlockSpec(memory_space=pltpu.VMEM)
    field = jax.ShapeDtypeStruct(level, f32)
    results = pl.pallas_call(
        functools.partial(kernel, tuple(scratch)),
        out_shape=(V(*level),) * 4,
        in_specs=[any_spec] * 7,
        out_specs=(vmem_spec,) * 4,
        scratch_shapes=list(scratch.values()),
        compiler_params=pltpu.CompilerParams(collective_id=0, has_side_effects=True),
    )(zonal, meridional, vertical, pressure, coupling, surface, lid_flag)
    return tuple(pl.pallas_call(
        store_kernel,
        out_shape=(field,) * 4,
        in_specs=[vmem_spec] * 4,
        out_specs=(any_spec,) * 4,
        scratch_shapes=[pltpu.SemaphoreType.DMA((4,))],
        compiler_params=pltpu.CompilerParams(vmem_limit_bytes=1 << 22),
    )(*results))


def solution(mesh):
    field = P("lev", "gx", "gy")
    plane = P("gx", "gy")
    return jax.shard_map(
        body, mesh=mesh,
        in_specs=(field,) * 5 + (plane,) * 2,
        out_specs=(field,) * 4,
        check_vma=False,
    )
```

```python
import functools
import types

import jax
import jax.numpy as jnp
from jax import lax
from jax.experimental import pallas as pl
from jax.experimental.pallas import tpu as pltpu
from jax.sharding import PartitionSpec as P

SUBSTEPS = 3
MESH = pl.DeviceIdType.MESH
PAD = 8
GROUPS = 4
EDGES = FIRST = 0
ROWS = EDGES + SUBSTEPS
EXTRA = ROWS + SUBSTEPS
STATIC = EXTRA + SUBSTEPS - 1


def inverse(d1, d2, d3, q1, q2):
    m1 = d2 * d3 - q2 * q2
    whole = 1.0 / (d1 * m1 - q1 * q1 * d3)
    n12 = q1 * d3 * whole
    n13 = q1 * q2 * whole
    n23 = d1 * q2 * whole
    return (
        (m1 * whole, n12, n13),
        (n12, d1 * d3 * whole, n23),
        (n13, n23, (d1 * d2 - q1 * q1) * whole),
    )


def face_row(rows, col, face):
    return jnp.where(face == 1, rows[0][col], jnp.where(
        face == 2, rows[1][col], jnp.where(face == 3, rows[2][col], 0.0)))


def kernel(names, zon, mer, ver, pre, cou, sur, lid, out_u, out_v, out_w, out_p, *scratch):
    m = types.SimpleNamespace(**dict(zip(names, scratch)))
    us, vs, ws, ps, cs = m.us, m.vs, m.ws, m.ps, m.cs
    L, I, J = zon.shape
    g = lax.axis_index("lev")
    gx = lax.axis_index("gx")
    gy = lax.axis_index("gy")
    nx = lax.axis_size("gx")
    ny = lax.axis_size("gy")
    groups = GROUPS
    x_dev = ({"gx": lax.rem(gx + nx - 1, nx)}, {"gx": lax.rem(gx + 1, nx)})
    y_dev = ({"gy": lax.rem(gy + ny - 1, ny)}, {"gy": lax.rem(gy + 1, ny)})
    peers = [{"lev": lax.rem(g + d, groups)} for d in range(1, groups)]
    around = [{**dev, "lev": lax.rem(g + d, groups)}
              for d in range(groups) for dev in x_dev + y_dev]
    inner = pl.ds(PAD, I)

    loads = [
        pltpu.make_async_copy(src, dst, m.load_sem.at[n])
        for n, (src, dst) in enumerate([
            (pre, ps.at[:, inner, :]),
            (mer, vs),
            (zon, us.at[:, inner, :]),
            (cou, cs.at[pl.ds(0, L)]),
            (sur, m.ks),
            (lid, m.ls),
            (ver, ws),
        ])
    ]
    barrier = pltpu.get_barrier_semaphore()
    everyone = around[:4] + peers + around[4:]
    for n, dev in enumerate(everyone):
        pl.semaphore_signal(barrier, inc=1, device_id=dev, device_id_type=MESH)
        if n == 6:
            for copy in loads:
                copy.start()

    lane = lax.broadcasted_iota(jnp.int32, (I, J), 1)
    level = lax.broadcasted_iota(jnp.int32, (L, J), 0)
    quad = lane // 4
    sub = lane % 4
    edge = (lane < 2) | (lane >= J - 2)
    lane8 = lax.broadcasted_iota(jnp.int32, (8, J), 1)
    quad8 = lane8 // 4
    lane4 = lax.broadcasted_iota(jnp.int32, (4, J), 1)
    live8 = (quad8 % 4 == 0) & (quad8 < 16)
    zero = jnp.zeros((I, J), jnp.float32)
    def remote(src, dst, dev, slot, send=0):
        return pltpu.make_async_remote_copy(
            src_ref=src, dst_ref=dst, send_sem=m.send_sem.at[send], recv_sem=m.recv_sem.at[slot],
            device_id=dev, device_id_type=MESH)

    middle = (g == 1) | (g == 2)
    rows_sent = []

    def count(ref):
        rows = 1
        for size in ref.shape[:-1]:
            rows *= size
        return rows

    def start(slot, copies):
        rows = 0
        for src, dst, dev in copies:
            remote(src, dst, dev, slot).start()
            rows += count(src)
        rows_sent.append(rows)
        return rows

    def arrive(sem, rows):
        block = m.tally.at[pl.ds(0, rows)]
        pltpu.make_async_copy(block, block, sem).wait()

    def side_row(side, r):
        return r if side == 0 else I - 2 + r

    def packed(k, plane, held):
        return jnp.where(quad == k, pltpu.roll(plane, 4 * k + 2, 1), held)

    def strips(phase, slot, planes):
        tile = jnp.zeros((8, J), jnp.float32)
        for n, plane in enumerate(planes):
            m.xsi[phase, 0, pl.ds(2 * n, 2), :] = plane[0:2]
            m.xsi[phase, 1, pl.ds(2 * n, 2), :] = plane[I - 2:I]
            for v in range(4):
                turned = pltpu.roll(plane[8 * v:8 * v + 8], 16 * v + 4 * n + 2, 1)
                tile = jnp.where(quad8 == 4 * v + n, turned, tile)
        m.ysi[phase] = jnp.where(lane4 < 64, tile[0:4], pltpu.roll(tile[4:8], 64, 1))
        return start(slot, [
            copy
            for d in range(groups) for side in range(2)
            for copy in (
                (m.xsi.at[phase, side], m.xri.at[phase, 1 - side, g], around[4 * d + side]),
                (m.ysi.at[phase], m.yri.at[phase, 1 - side, g], around[4 * d + 2 + side]),
            )
        ])

    def x_rows(phase, side, h, n):
        return m.xri[phase, side, h, pl.ds(2 * n, 2), :]

    def y_tile(phase, h):
        half = jnp.where(lane4 % 4 < 2, m.yri[phase, 0, h], m.yri[phase, 1, h])
        return jnp.concatenate([half, pltpu.roll(half, 64, 1)], 0)

    def turn8(tile, n):
        return pltpu.roll(tile, J - 4 * n, 1) if n else tile

    for step in range(SUBSTEPS - 1):
        m.lex[step] = zero
    loads[0].wait()
    for side in range(2):
        for r in range(2):
            m.xs0[side, pl.ds(r * L, L), :] = ps[:, PAD + side_row(side, r), :]
    pack = lax.fori_loop(0, L, lambda k, acc: packed(k, ps[k, inner, :], acc), zero, unroll=16)
    m.ys0[0] = pack
    loads[1].wait()
    pack_v = lax.fori_loop(0, L, lambda k, acc: packed(k, vs[k], acc), zero, unroll=16)
    m.ys0[1] = pack_v
    loads[2].wait()
    for side in range(2):
        m.xs0[side, pl.ds(2 * L, L), :] = us[:, PAD + (I - 1) * side, :]
    for n in range(3, 6):
        loads[n].wait()

    pl.semaphore_wait(barrier, len(everyone))
    messages = start(FIRST, [
        (m.xs0.at[0], m.xr0.at[1], x_dev[0]),
        (m.xs0.at[1], m.xr0.at[0], x_dev[1]),
        (m.ys0, m.yr0.at[1], y_dev[0]),
        (m.ys0, m.yr0.at[0], y_dev[1]),
        (cs.at[0], m.cup, peers[-1]),
    ])

    halo_rows = jnp.zeros((L, PAD, J), jnp.float32)
    for ref in (ps, us):
        ref[:, 0:PAD, :] = halo_rows
        ref[:, PAD + I:, :] = halo_rows

    cs[L] = zero
    height = m.ks[...] - g * L
    lid_here = jnp.where(g == groups - 1, m.ls[...].astype(jnp.float32), 0.0)
    is_first = jnp.where(g == 0, 1.0, 0.0).astype(jnp.float32)
    above_sign = jnp.where(g == groups - 1, 0.0, -1.0).astype(jnp.float32)
    g_below = lax.rem(g + groups - 1, groups)

    def factor(k, held):
        rate, z = held
        here = cs[k]
        above = cs[k + 1]
        keep = height <= k
        delta = 1.0 + here * rate + jnp.where(k == L - 1, lid_here * here, 0.0)
        one = 1.0 / (delta + above)
        rate = jnp.where(keep, delta * one, 1.0)
        one = jnp.where(keep, one, 0.0)
        a = here * one
        z = jnp.where(k == 0, one, a * z)
        m.im[k] = one
        m.am[k] = a
        m.gm[k] = above * one
        m.gf[k] = z
        return rate, z

    lax.fori_loop(0, L, factor, (zero + is_first, zero), unroll=4)

    def respond(n, held):
        a, b = held
        k = L - 1 - n
        up = m.gm[k]
        a = m.gf[k] + up * a
        b = jnp.where(n == 0, m.im[L - 1], up * b)
        m.gf[k] = a
        m.gl[k] = b
        return a, b

    lax.fori_loop(0, L, respond, (zero, zero), unroll=4)
    own_inv = 1.0 / cs[0]
    own_static = (m.gf[0] + own_inv, m.gf[L - 1], m.gl[L - 1])
    for n in range(3):
        m.sta[g, n] = own_static[n]
    static = start(STATIC, [(m.sta.at[g], m.sta.at[g], dev) for dev in peers])
    static += strips(0, STATIC, own_static)

    def slopes(k, held):
        f_before, l_before, a_pack, b_pack = held
        f = m.gf[k]
        l = m.gl[k]
        a = jnp.where(k == 0, (is_first - 1.0) * 0.5 * own_inv, 0.5 * (f - f_before))
        b = jnp.where(k == 0, is_first * -0.5 * l, -0.5 * (l - l_before))
        m.aa[k] = a
        m.bb[k] = b
        return f, l, packed(k, a, a_pack), packed(k, b, b_pack)

    unused_f, unused_l, a_pack, b_pack = lax.fori_loop(0, L, slopes, (zero,) * 4, unroll=8)
    m.ysa[0] = a_pack
    m.ysa[1] = b_pack
    for side in range(2):
        for r in range(2):
            m.xsa[side, pl.ds(r * L, L), :] = m.aa[:, side_row(side, r), :]
            m.xsa[side, pl.ds((2 + r) * L, L), :] = m.bb[:, side_row(side, r), :]
    static += start(STATIC, [
        (m.xsa.at[0], m.xra.at[1], x_dev[0]),
        (m.xsa.at[1], m.xra.at[0], x_dev[1]),
        (m.ysa, m.yra.at[1], y_dev[0]),
        (m.ysa, m.yra.at[0], y_dev[1]),
    ])

    pick = lax.broadcasted_iota(jnp.int32, (J, 4 * J), 0)
    into = lax.broadcasted_iota(jnp.int32, (J, 4 * J), 1)
    m.sel[...] = jnp.where(
        (pick % 16 == into % 4) & (pick // 16 == into // J), 1.0, 0.0).astype(jnp.bfloat16)

    def predict(step, k, _):
        here = ps[k, inner, :]
        force = 0.0625 * (
            ps[k, pl.ds(PAD + 2, I), :] + ps[k, pl.ds(PAD - 2, I), :]
            + pltpu.roll(here, J - 2, 1) + pltpu.roll(here, 2, 1) - 4.0 * here)
        if step == 0:
            v = vs[k]
            force = force - 0.25 * (
                us[k, pl.ds(PAD + 1, I), :] - us[k, pl.ds(PAD - 1, I), :]
                + pltpu.roll(v, J - 1, 1) - pltpu.roll(v, 1, 1))
        else:
            force = force + m.fs[k]
        m.fs[k] = force
        m.pp[k + 1] = here + force
        return 0

    lax.fori_loop(0, L, functools.partial(predict, 0), 0, unroll=16)
    loads[6].wait()

    up_inv = zero
    for step in range(SUBSTEPS):
        last = step == SUBSTEPS - 1
        arrive(m.recv_sem.at[EDGES + step], messages)
        rows = []
        if step == 0:
            for side in range(2):
                rows += [m.xr0[side, pl.ds(r * L, L), :] for r in range(2)]
            diff = jnp.where(sub < 2, m.yr0[0, 0], m.yr0[1, 0]) - pack
            drift = jnp.where(sub < 2, m.yr0[0, 1], m.yr0[1, 1]) - pack_v
            spin = jnp.where(sub == 1, pltpu.roll(drift, J - 1, 1),
                             jnp.where(sub == 2, -pltpu.roll(drift, 1, 1), 0.0))
            up_inv = 1.0 / m.cup[...]
        else:
            for side in range(2):
                jumps = [x_rows(step, side, h, 0) - x_rows(step, side, h - 1, 1) for h in (1, 2, 3)]
                lower = sum(m.nx[side, n, 0:2, :] * jumps[n] for n in range(3))
                upper = sum(m.nx[side, 3 + n, 0:2, :] * jumps[n] for n in range(3))
                floor = lower + 0.5 * x_rows(step, side, g_below, 2)
                for r in range(2):
                    low_r = jnp.where(level == 0, floor[r:r + 1], lower[r:r + 1])
                    rows.append(
                        m.xr[step - 1, side, pl.ds(r * L, L), :]
                        + m.xra[side, pl.ds(r * L, L), :] * low_r
                        + m.xra[side, pl.ds((2 + r) * L, L), :] * upper[r:r + 1])
            tiles = [y_tile(step, h) for h in range(groups)]
            jumps = [tiles[h] - turn8(tiles[h - 1], 1) for h in (1, 2, 3)]
            lower = sum(m.ny[n] * jumps[n] for n in range(3))
            upper = sum(m.ny[3 + n] * jumps[n] for n in range(3))
            floor = jnp.where(live8, lower + 0.5 * turn8(y_tile(step, g_below), 2), 0.0)
            whole = jnp.concatenate([lower, upper, floor], 0)
            coarse = whole.astype(jnp.bfloat16)
            rest = whole - coarse.astype(jnp.float32)
            second = rest.astype(jnp.bfloat16)
            fine = (rest - second.astype(jnp.float32)).astype(jnp.bfloat16)
            wide = (jnp.dot(fine, m.sel[...], preferred_element_type=jnp.float32)
                    + jnp.dot(second, m.sel[...], preferred_element_type=jnp.float32)
                    + jnp.dot(coarse, m.sel[...], preferred_element_type=jnp.float32))
            parts = [jnp.concatenate([wide[8 * n:8 * n + 8, J * v:J * v + J] for v in range(4)], 0)
                     for n in range(3)]
            diff = (jnp.where(sub < 2, m.yr[step - 1, 0], m.yr[step - 1, 1])
                    + m.am2[...] * jnp.where(quad == 0, parts[2], parts[0])
                    + m.bm2[...] * parts[1]) - pack
        mend2 = 0.0625 * jnp.where(sub < 2, pltpu.roll(diff, J - 2, 1), pltpu.roll(diff, 2, 1))
        mend1 = jnp.where(sub == 1, pltpu.roll(diff, J - 1, 1),
                          jnp.where(sub == 2, -pltpu.roll(diff, 1, 1), 0.0))
        adds = [0.0625 * row for row in rows]
        if step == 0:
            mend2 = mend2 - 0.25 * spin
            adds[0] = adds[0] + 0.25 * m.xr0[0, pl.ds(2 * L, L), :]
            adds[3] = adds[3] - 0.25 * m.xr0[1, pl.ds(2 * L, L), :]
        for at, add in zip((0, 1, I - 2, I - 1), adds):
            m.fs[:, at, :] = m.fs[:, at, :] + add
            m.pp[pl.ds(1, L), at, :] = m.pp[pl.ds(1, L), at, :] + add
        m.hx[0] = rows[1]
        m.hx[1] = rows[2]

        def eliminate(k, z, mid_above, mid_below):
            z = (ws[k] - 0.5 * (mid_above - mid_below)) * m.im[k] + m.am[k] * z
            m.zz[k] = z
            return z

        def forward(k, held):
            z, one_below, two_below = held
            fix = jnp.where(edge, pltpu.roll(mend2, J - 2 - 4 * k, 1), 0.0)
            m.fs[k] = m.fs[k] + fix
            here = m.pp[k + 1] + fix
            m.pp[k + 1] = here
            z = eliminate(jnp.maximum(k - 1, 0), z, here, two_below)
            z = jnp.where(k == 0, 0.0, z)
            one_below = jnp.where(k == 0, (is_first - 1.0) * here, one_below)
            return z, here, one_below

        z, top, under_top = lax.fori_loop(0, L, forward, (zero,) * 3, unroll=16)
        m.pls[step] = top
        group_rows = start(ROWS + step, [(m.pls.at[step], m.plr.at[step], peers[0])])
        eliminate(L - 1, z, above_sign * top, under_top)
        low = m.pp[1]

        def backward(n, y):
            k = L - 1 - n
            y = m.zz[k] + m.gm[k] * y
            m.zz[k] = y
            return y

        y_low = lax.fori_loop(0, L, backward, zero, unroll=8)
        down = y_low - 0.5 * low * own_inv
        up = m.zz[L - 1] + 0.5 * top * up_inv
        if step == 0:
            m.lev[g, 0] = down
            m.lev[g, 1] = up
            group_rows += start(ROWS, [(m.lev.at[g], m.lev.at[g], dev) for dev in peers])
            messages = strips(1, EDGES + 1, (down, up, top))
        else:
            if not last:
                messages = strips(step + 1, EDGES + step + 1, (down, up, top))
            for d in range(3):
                m.lvs[step - 1, d] = m.mix[0, d] * down + m.mix[1, d] * up
            group_rows += start(ROWS + step, [
                (m.lvs.at[step - 1, d], m.lvr.at[step - 1, d], peers[d]) for d in range(3)])
            m.les[step - 1] = up
            extra = remote(m.les.at[step - 1], m.lex.at[step - 1], {"lev": groups - 1 - g},
                           EXTRA + step - 1, step)
            pl.when(middle)(extra.start)

        def plain(k, held):
            before, acc = held
            y = m.zz[k]
            q = m.pp[k + 1] - 0.5 * (y - before)
            m.qs[k] = q
            return y, acc if last else packed(k, q, acc)

        ghost = y_low - (is_first * y_low - m.aa[0] * low)
        unused_y, q_pack = lax.fori_loop(0, L, plain, (ghost, zero), unroll=16)
        if not last:
            for side in range(2):
                for r in range(2):
                    m.xs[step, side, pl.ds(r * L, L), :] = m.qs[:, side_row(side, r), :]
            m.ys[step] = q_pack
            messages += start(EDGES + step + 1, [
                (m.xs.at[step, 0], m.xr.at[step, 1], x_dev[0]),
                (m.xs.at[step, 1], m.xr.at[step, 0], x_dev[1]),
                (m.ys.at[step], m.yr.at[step, 1], y_dev[0]),
                (m.ys.at[step], m.yr.at[step, 0], y_dev[1]),
            ])


        def move(k, _):
            here = ps[k, inner, :]
            fix = jnp.where(edge, pltpu.roll(mend1, J - 2 - 4 * k, 1), 0.0)
            new_u = us[k, inner, :] - 0.25 * (
                ps[k, pl.ds(PAD + 1, I), :] - ps[k, pl.ds(PAD - 1, I), :])
            new_v = vs[k] - 0.25 * (
                pltpu.roll(here, J - 1, 1) - pltpu.roll(here, 1, 1) + fix)
            if last:
                out_u[k] = new_u
                out_v[k] = new_v
            else:
                us[k, inner, :] = new_u
                vs[k] = new_v
            return 0

        lax.fori_loop(0, L, move, 0, unroll=8)
        for end, at in ((0, 0), (1, I - 1)):
            kick = (0.25 - 0.5 * end) * m.hx[end]
            if last:
                out_u[:, at, :] = out_u[:, at, :] + kick
            else:
                us[:, PAD + at, :] = us[:, PAD + at, :] + kick

        if step == 0:
            arrive(m.recv_sem.at[STATIC], static)
            sta = m.sta
            rows_of = inverse(sta[1, 0] + sta[0, 2], sta[2, 0] + sta[1, 2], sta[3, 0] + sta[2, 2],
                              sta[1, 1], sta[2, 1])
            for slot in range(2):
                face = g + slot
                row = [face_row(rows_of, col, face) for col in range(3)]
                for col in range(3):
                    m.inv[slot, col] = row[col]
                mine = jnp.where((face >= 1) & (face <= 3), 1.0, 0.0).astype(jnp.float32)

                def of(h):
                    return jnp.where(h == 1, row[0], jnp.where(h == 2, row[1], row[2]))

                for d in range(3):
                    o = lax.rem(g + groups - 1 - d, groups)
                    m.cw[slot, d] = jnp.where(o == 0, -row[0], jnp.where(
                        o == groups - 1, row[2], jnp.where(middle, of(o), mine)))
                m.cw[slot, 3] = jnp.where(g == 0, 0.0, of(g))
                m.cw[slot, 4] = jnp.where(g == groups - 1, 0.0, -of(g + 1))
                m.cw[slot, 5] = jnp.where(middle, -of(groups - g), 0.0)
            for d in range(3):
                to = lax.rem(g + 1 + d, groups)
                row = [jnp.where(to == 0, rows_of[0][col], rows_of[2][col]) for col in range(3)]
                raw = (to == 1) | (to == 2)
                m.mix[0, d] = jnp.where(g == 0, 0.0, jnp.where((g == groups - 1) | raw, 1.0, jnp.where(
                    g == 1, row[0], row[1])))
                m.mix[1, d] = jnp.where(g == 0, 1.0, jnp.where((g == groups - 1) | raw, 0.0, jnp.where(
                    g == 1, -row[1], -row[2])))
            for side in range(2):
                part = lambda h, n: x_rows(0, side, h, n)
                rows_of = inverse(part(1, 0) + part(0, 2), part(2, 0) + part(1, 2),
                                  part(3, 0) + part(2, 2), part(1, 1), part(2, 1))
                for slot in range(2):
                    for col in range(3):
                        m.nx[side, 3 * slot + col, 0:2, :] = face_row(rows_of, col, g + slot)
            tiles = [y_tile(0, h) for h in range(groups)]
            part = lambda h, n: jnp.where(live8, turn8(tiles[h], n), 1.0)
            rows_of = inverse(part(1, 0) + part(0, 2), part(2, 0) + part(1, 2),
                              part(3, 0) + part(2, 2), part(1, 1), part(2, 1))
            for slot in range(2):
                for col in range(3):
                    m.ny[3 * slot + col] = jnp.where(live8, face_row(rows_of, col, g + slot), 0.0)
            m.am2[...] = jnp.where(sub < 2, m.yra[0, 0], m.yra[1, 0])
            m.bm2[...] = jnp.where(sub < 2, m.yra[0, 1], m.yra[1, 1])

        arrive(m.recv_sem.at[ROWS + step], group_rows)
        if step == 0:
            jumps = [m.lev[h, 0] - m.lev[h - 1, 1] for h in (1, 2, 3)]
            under = sum(m.inv[0, n] * jumps[n] for n in range(3))
            over = sum(m.inv[1, n] * jumps[n] for n in range(3))
        else:
            pl.when(middle)(extra.wait)
            terms = [m.lvr[step - 1, d] for d in range(3)] + [down, up, m.lex[step - 1]]
            under = sum(m.cw[0, n] * terms[n] for n in range(6))
            over = sum(m.cw[1, n] * terms[n] for n in range(6))
        under0 = under + 0.5 * m.plr[step]

        def correct(k, acc):
            x = m.zz[k] - m.gf[k] * under + m.gl[k] * over
            new = m.qs[k] + m.aa[k] * jnp.where(k == 0, under0, under) + m.bb[k] * over
            if last:
                out_w[k] = x
                out_p[k] = new
                return acc
            ws[k] = x
            ps[k, inner, :] = new
            return packed(k, new, acc)

        pack = lax.fori_loop(0, L, correct, zero, unroll=16)
        if not last:
            lax.fori_loop(0, L, functools.partial(predict, step + 1), 0, unroll=16)

    arrive(m.send_sem.at[0], sum(rows_sent))


def store_kernel(*refs):
    sem = refs[-1]
    copies = [
        pltpu.make_async_copy(refs[n], refs[4 + n], sem.at[n]) for n in range(4)
    ]
    for copy in copies:
        copy.start()
    for copy in copies:
        copy.wait()


def body(zonal, meridional, vertical, pressure, coupling, surface, lid_flag):
    L, I, J = zonal.shape
    IP = I + 2 * PAD
    S = SUBSTEPS
    G = GROUPS
    f32 = jnp.float32
    V = lambda *shape: pltpu.VMEM(shape, f32)
    level = (L, I, J)
    scratch = dict(
        us=V(L, IP, J), vs=V(*level), ws=V(*level), ps=V(L, IP, J), cs=V(L + 1, I, J),
        ks=pltpu.VMEM((I, J), jnp.int32), ls=pltpu.VMEM((I, J), jnp.int32),
        fs=V(*level), pp=V(L + 2, I, J), zz=V(*level), qs=V(*level),
        am=V(*level), im=V(*level), gm=V(*level), gf=V(*level), gl=V(*level),
        aa=V(*level), bb=V(*level),
        xs0=V(2, 3 * L, J), ys0=V(2, I, J), xr0=V(2, 3 * L, J), yr0=V(2, 2, I, J),
        xs=V(S - 1, 2, 2 * L, J), ys=V(S - 1, I, J),
        xr=V(S - 1, 2, 2 * L, J), yr=V(S - 1, 2, I, J),
        xsa=V(2, 4 * L, J), ysa=V(2, I, J), xra=V(2, 4 * L, J), yra=V(2, 2, I, J),
        xsi=V(S, 2, 6, J), ysi=V(S, 4, J), xri=V(S, 2, G, 6, J), yri=V(S, 2, G, 4, J),
        sta=V(G, 3, I, J), lev=V(G, 2, I, J), cup=V(I, J),
        lvs=V(S - 1, 3, I, J), lvr=V(S - 1, 3, I, J), les=V(S - 1, I, J), lex=V(S - 1, I, J),
        mix=V(2, 3, I, J), cw=V(2, 6, I, J), pls=V(S, I, J), plr=V(S, I, J), hx=V(2, L, J),
        inv=V(2, 3, I, J), nx=V(2, 6, 8, J), ny=V(6, 8, J), am2=V(I, J), bm2=V(I, J),
        sel=pltpu.VMEM((J, 4 * J), jnp.bfloat16),
        load_sem=pltpu.SemaphoreType.DMA((7,)),
        tally=V(2560, J),
        send_sem=pltpu.SemaphoreType.DMA((S,)),
        recv_sem=pltpu.SemaphoreType.DMA((STATIC + 1,)),
    )
    any_spec = pl.BlockSpec(memory_space=pl.ANY)
    vmem_spec = pl.BlockSpec(memory_space=pltpu.VMEM)
    field = jax.ShapeDtypeStruct(level, f32)
    results = pl.pallas_call(
        functools.partial(kernel, tuple(scratch)),
        out_shape=(V(*level),) * 4,
        in_specs=[any_spec] * 7,
        out_specs=(vmem_spec,) * 4,
        scratch_shapes=list(scratch.values()),
        compiler_params=pltpu.CompilerParams(collective_id=0, has_side_effects=True),
    )(zonal, meridional, vertical, pressure, coupling, surface, lid_flag)
    return tuple(pl.pallas_call(
        store_kernel,
        out_shape=(field,) * 4,
        in_specs=[vmem_spec] * 4,
        out_specs=(any_spec,) * 4,
        scratch_shapes=[pltpu.SemaphoreType.DMA((4,))],
        compiler_params=pltpu.CompilerParams(vmem_limit_bytes=1 << 22),
    )(*results))


def solution(mesh):
    field = P("lev", "gx", "gy")
    plane = P("gx", "gy")
    return jax.shard_map(
        body, mesh=mesh,
        in_specs=(field,) * 5 + (plane,) * 2,
        out_specs=(field,) * 4,
        check_vma=False,
    )
```

```python
import functools
import types

import jax
import jax.numpy as jnp
from jax import lax
from jax.experimental import pallas as pl
from jax.experimental.pallas import tpu as pltpu
from jax.sharding import PartitionSpec as P

SUBSTEPS = 3
MESH = pl.DeviceIdType.MESH
PAD = 8
GROUPS = 4
EDGES = FIRST = 0
ROWS = EDGES + SUBSTEPS
EXTRA = ROWS + SUBSTEPS
STATIC = EXTRA + SUBSTEPS - 1


def inverse(d1, d2, d3, q1, q2):
    m1 = d2 * d3 - q2 * q2
    whole = 1.0 / (d1 * m1 - q1 * q1 * d3)
    n12 = q1 * d3 * whole
    n13 = q1 * q2 * whole
    n23 = d1 * q2 * whole
    return (
        (m1 * whole, n12, n13),
        (n12, d1 * d3 * whole, n23),
        (n13, n23, (d1 * d2 - q1 * q1) * whole),
    )


def face_row(rows, col, face):
    return jnp.where(face == 1, rows[0][col], jnp.where(
        face == 2, rows[1][col], jnp.where(face == 3, rows[2][col], 0.0)))


def kernel(names, zon, mer, ver, pre, cou, sur, lid, out_u, out_v, out_w, out_p, *scratch):
    m = types.SimpleNamespace(**dict(zip(names, scratch)))
    us, vs, ws, ps, cs = m.us, m.vs, m.ws, m.ps, m.cs
    L, I, J = zon.shape
    g = lax.axis_index("lev")
    gx = lax.axis_index("gx")
    gy = lax.axis_index("gy")
    nx = lax.axis_size("gx")
    ny = lax.axis_size("gy")
    groups = GROUPS
    x_dev = ({"gx": lax.rem(gx + nx - 1, nx)}, {"gx": lax.rem(gx + 1, nx)})
    y_dev = ({"gy": lax.rem(gy + ny - 1, ny)}, {"gy": lax.rem(gy + 1, ny)})
    peers = [{"lev": lax.rem(g + d, groups)} for d in range(1, groups)]
    around = [{**dev, "lev": lax.rem(g + d, groups)}
              for d in range(groups) for dev in x_dev + y_dev]
    inner = pl.ds(PAD, I)

    loads = [
        pltpu.make_async_copy(src, dst, m.load_sem.at[n])
        for n, (src, dst) in enumerate([
            (pre, ps.at[:, inner, :]),
            (mer, vs),
            (zon, us.at[:, inner, :]),
            (cou, cs.at[pl.ds(0, L)]),
            (sur, m.ks),
            (lid, m.ls),
            (ver, ws),
        ])
    ]
    barrier = pltpu.get_barrier_semaphore()
    near = around[:4] + peers
    for dev in near:
        pl.semaphore_signal(barrier, inc=1, device_id=dev, device_id_type=MESH)
    for copy in loads:
        copy.start()

    lane = lax.broadcasted_iota(jnp.int32, (I, J), 1)
    level = lax.broadcasted_iota(jnp.int32, (L, J), 0)
    quad = lane // 4
    sub = lane % 4
    edge = (lane < 2) | (lane >= J - 2)
    lane8 = lax.broadcasted_iota(jnp.int32, (8, J), 1)
    quad8 = lane8 // 4
    lane4 = lax.broadcasted_iota(jnp.int32, (4, J), 1)
    live8 = (quad8 % 4 == 0) & (quad8 < 16)
    zero = jnp.zeros((I, J), jnp.float32)
    def remote(src, dst, dev, slot, send=0):
        return pltpu.make_async_remote_copy(
            src_ref=src, dst_ref=dst, send_sem=m.send_sem.at[send], recv_sem=m.recv_sem.at[slot],
            device_id=dev, device_id_type=MESH)

    middle = (g == 1) | (g == 2)
    rows_sent = []

    def count(ref):
        rows = 1
        for size in ref.shape[:-1]:
            rows *= size
        return rows

    def start(slot, copies):
        rows = 0
        for src, dst, dev in copies:
            remote(src, dst, dev, slot).start()
            rows += count(src)
        rows_sent.append(rows)
        return rows

    def arrive(sem, rows):
        block = m.tally.at[pl.ds(0, rows)]
        pltpu.make_async_copy(block, block, sem).wait()

    def side_row(side, r):
        return r if side == 0 else I - 2 + r

    def packed(k, plane, held):
        return jnp.where(quad == k, pltpu.roll(plane, 4 * k + 2, 1), held)

    def swapped(held):
        return jnp.where(sub < 2, pltpu.roll(held, J - 2, 1), pltpu.roll(held, 2, 1))

    def strips(phase, slot, planes):
        tile = jnp.zeros((8, J), jnp.float32)
        for n, plane in enumerate(planes):
            m.xsi[phase, 0, pl.ds(2 * n, 2), :] = plane[0:2]
            m.xsi[phase, 1, pl.ds(2 * n, 2), :] = plane[I - 2:I]
            for v in range(4):
                turned = pltpu.roll(plane[8 * v:8 * v + 8], 16 * v + 4 * n + 2, 1)
                tile = jnp.where(quad8 == 4 * v + n, turned, tile)
        m.ysi[phase] = jnp.where(lane4 < 64, tile[0:4], pltpu.roll(tile[4:8], 64, 1))
        return start(slot, [
            copy
            for d in range(groups) for side in range(2)
            for copy in (
                (m.xsi.at[phase, side], m.xri.at[phase, 1 - side, g], around[4 * d + side]),
                (m.ysi.at[phase], m.yri.at[phase, 1 - side, g], around[4 * d + 2 + side]),
            )
        ])

    def x_rows(phase, side, h, n):
        return m.xri[phase, side, h, pl.ds(2 * n, 2), :]

    def y_tile(phase, h):
        half = jnp.where(lane4 % 4 < 2, m.yri[phase, 0, h], m.yri[phase, 1, h])
        return jnp.concatenate([half, pltpu.roll(half, 64, 1)], 0)

    def turn8(tile, n):
        return pltpu.roll(tile, J - 4 * n, 1) if n else tile

    for step in range(SUBSTEPS - 1):
        m.lex[step] = zero
    loads[0].wait()
    for side in range(2):
        for r in range(2):
            m.xs0[side, pl.ds(r * L, L), :] = ps[:, PAD + side_row(side, r), :]
    pack = lax.fori_loop(0, L, lambda k, acc: packed(k, ps[k, inner, :], acc), zero, unroll=16)
    m.ys0[0] = pack
    loads[1].wait()
    pack_v = lax.fori_loop(0, L, lambda k, acc: packed(k, vs[k], acc), zero, unroll=16)
    m.ys0[1] = pack_v
    loads[2].wait()
    for side in range(2):
        m.xs0[side, pl.ds(2 * L, L), :] = us[:, PAD + (I - 1) * side, :]
    for n in range(3, 6):
        loads[n].wait()

    pl.semaphore_wait(barrier, len(near))
    for dev in around[:4]:
        pl.semaphore_signal(m.hood, inc=1, device_id=dev, device_id_type=MESH)
    messages = start(FIRST, [
        (m.xs0.at[0], m.xr0.at[1], x_dev[0]),
        (m.xs0.at[1], m.xr0.at[0], x_dev[1]),
        (m.ys0, m.yr0.at[1], y_dev[0]),
        (m.ys0, m.yr0.at[0], y_dev[1]),
        (cs.at[0], m.cup, peers[-1]),
    ])

    halo_rows = jnp.zeros((L, PAD, J), jnp.float32)
    for ref in (ps, us):
        ref[:, 0:PAD, :] = halo_rows
        ref[:, PAD + I:, :] = halo_rows

    cs[L] = zero
    height = m.ks[...] - g * L
    lid_here = jnp.where(g == groups - 1, m.ls[...].astype(jnp.float32), 0.0)
    is_first = jnp.where(g == 0, 1.0, 0.0).astype(jnp.float32)
    above_sign = jnp.where(g == groups - 1, 0.0, -1.0).astype(jnp.float32)
    g_below = lax.rem(g + groups - 1, groups)

    def factor(k, held):
        rate, z = held
        here = cs[k]
        above = cs[k + 1]
        keep = height <= k
        delta = 1.0 + here * rate + jnp.where(k == L - 1, lid_here * here, 0.0)
        one = 1.0 / (delta + above)
        rate = jnp.where(keep, delta * one, 1.0)
        one = jnp.where(keep, one, 0.0)
        a = here * one
        z = jnp.where(k == 0, one, a * z)
        m.im[k] = one
        m.am[k] = a
        m.gm[k] = above * one
        m.gf[k] = z
        return rate, z

    lax.fori_loop(0, L, factor, (zero + is_first, zero), unroll=4)

    def respond(n, held):
        a, b = held
        k = L - 1 - n
        up = m.gm[k]
        a = m.gf[k] + up * a
        b = jnp.where(n == 0, m.im[L - 1], up * b)
        m.gf[k] = a
        m.gl[k] = b
        return a, b

    lax.fori_loop(0, L, respond, (zero, zero), unroll=4)
    own_inv = 1.0 / cs[0]
    own_static = (m.gf[0] + own_inv, m.gf[L - 1], m.gl[L - 1])
    for n in range(3):
        m.sta[g, n] = own_static[n]
    static = start(STATIC, [(m.sta.at[g], m.sta.at[g], dev) for dev in peers])


    def slopes(k, held):
        f_before, l_before, a_pack, b_pack = held
        f = m.gf[k]
        l = m.gl[k]
        a = jnp.where(k == 0, (is_first - 1.0) * 0.5 * own_inv, 0.5 * (f - f_before))
        b = jnp.where(k == 0, is_first * -0.5 * l, -0.5 * (l - l_before))
        m.aa[k] = a
        m.bb[k] = b
        return f, l, packed(k, a, a_pack), packed(k, b, b_pack)

    unused_f, unused_l, a_pack, b_pack = lax.fori_loop(0, L, slopes, (zero,) * 4, unroll=8)
    m.ysa[0] = a_pack
    m.ysa[1] = b_pack
    for side in range(2):
        for r in range(2):
            m.xsa[side, pl.ds(r * L, L), :] = m.aa[:, side_row(side, r), :]
            m.xsa[side, pl.ds((2 + r) * L, L), :] = m.bb[:, side_row(side, r), :]
    static += start(STATIC, [
        (m.xsa.at[0], m.xra.at[1], x_dev[0]),
        (m.xsa.at[1], m.xra.at[0], x_dev[1]),
        (m.ysa, m.yra.at[1], y_dev[0]),
        (m.ysa, m.yra.at[0], y_dev[1]),
    ])

    pick = lax.broadcasted_iota(jnp.int32, (J, 4 * J), 0)
    into = lax.broadcasted_iota(jnp.int32, (J, 4 * J), 1)
    m.sel[...] = jnp.where(
        (pick % 16 == (into + 2) % 4) & (pick // 16 == into // J), 1.0, 0.0).astype(jnp.bfloat16)

    def predict(step, k, _):
        here = ps[k, inner, :]
        force = 0.0625 * (
            ps[k, pl.ds(PAD + 2, I), :] + ps[k, pl.ds(PAD - 2, I), :]
            + pltpu.roll(here, J - 2, 1) + pltpu.roll(here, 2, 1) - 4.0 * here)
        if step == 0:
            v = vs[k]
            force = force - 0.25 * (
                us[k, pl.ds(PAD + 1, I), :] - us[k, pl.ds(PAD - 1, I), :]
                + pltpu.roll(v, J - 1, 1) - pltpu.roll(v, 1, 1))
        else:
            force = force + m.fs[k]
        m.fs[k] = force
        m.pp[k + 1] = here + force
        return 0

    lax.fori_loop(0, L, functools.partial(predict, 0), 0, unroll=16)
    loads[6].wait()
    pl.semaphore_wait(m.hood, 4)
    static += strips(0, STATIC, [m.sta[g, n] for n in range(3)])

    up_inv = zero
    for step in range(SUBSTEPS):
        last = step == SUBSTEPS - 1
        arrive(m.recv_sem.at[EDGES + step], messages)
        rows = []
        if step == 0:
            for side in range(2):
                rows += [m.xr0[side, pl.ds(r * L, L), :] for r in range(2)]
            diff = swapped(jnp.where(sub < 2, m.yr0[0, 0], m.yr0[1, 0]) - pack)
            drift = jnp.where(sub < 2, m.yr0[0, 1], m.yr0[1, 1]) - pack_v
            spin = jnp.where(sub == 1, pltpu.roll(drift, J - 1, 1),
                             jnp.where(sub == 2, -pltpu.roll(drift, 1, 1), 0.0))
            up_inv = 1.0 / m.cup[...]
        else:
            for side in range(2):
                jumps = [x_rows(step, side, h, 0) - x_rows(step, side, h - 1, 1) for h in (1, 2, 3)]
                lower = sum(m.nx[side, n, 0:2, :] * jumps[n] for n in range(3))
                upper = sum(m.nx[side, 3 + n, 0:2, :] * jumps[n] for n in range(3))
                floor = lower + 0.5 * x_rows(step, side, g_below, 2)
                for r in range(2):
                    low_r = jnp.where(level == 0, floor[r:r + 1], lower[r:r + 1])
                    rows.append(
                        m.xr[step - 1, side, pl.ds(r * L, L), :]
                        + m.xra[side, pl.ds(r * L, L), :] * low_r
                        + m.xra[side, pl.ds((2 + r) * L, L), :] * upper[r:r + 1])
            tiles = [y_tile(step, h) for h in range(groups)]
            jumps = [tiles[h] - turn8(tiles[h - 1], 1) for h in (1, 2, 3)]
            lower = sum(m.ny[n] * jumps[n] for n in range(3))
            upper = sum(m.ny[3 + n] * jumps[n] for n in range(3))
            floor = jnp.where(live8, lower + 0.5 * turn8(y_tile(step, g_below), 2), 0.0)
            whole = jnp.concatenate([lower, upper, floor], 0)
            coarse = whole.astype(jnp.bfloat16)
            rest = whole - coarse.astype(jnp.float32)
            second = rest.astype(jnp.bfloat16)
            fine = (rest - second.astype(jnp.float32)).astype(jnp.bfloat16)
            wide = (jnp.dot(fine, m.sel[...], preferred_element_type=jnp.float32)
                    + jnp.dot(second, m.sel[...], preferred_element_type=jnp.float32)
                    + jnp.dot(coarse, m.sel[...], preferred_element_type=jnp.float32))
            parts = [jnp.concatenate([wide[8 * n:8 * n + 8, J * v:J * v + J] for v in range(4)], 0)
                     for n in range(3)]
            diff = (swapped(jnp.where(sub < 2, m.yr[step - 1, 0], m.yr[step - 1, 1]) - pack)
                    + m.am2[...] * jnp.where(quad == 0, parts[2], parts[0])
                    + m.bm2[...] * parts[1])
        mend2 = 0.0625 * diff
        mend1 = jnp.where(sub == 1, pltpu.roll(diff, 1, 1),
                          jnp.where(sub == 2, -pltpu.roll(diff, J - 1, 1), 0.0))
        adds = [0.0625 * row for row in rows]
        if step == 0:
            mend2 = mend2 - 0.25 * spin
            adds[0] = adds[0] + 0.25 * m.xr0[0, pl.ds(2 * L, L), :]
            adds[3] = adds[3] - 0.25 * m.xr0[1, pl.ds(2 * L, L), :]
        for at, add in zip((0, 1, I - 2, I - 1), adds):
            m.fs[:, at, :] = m.fs[:, at, :] + add
            m.pp[pl.ds(1, L), at, :] = m.pp[pl.ds(1, L), at, :] + add
        m.hx[0] = rows[1]
        m.hx[1] = rows[2]

        def eliminate(k, z, mid_above, mid_below):
            z = (ws[k] - 0.5 * (mid_above - mid_below)) * m.im[k] + m.am[k] * z
            m.zz[k] = z
            return z

        def forward(k, held):
            z, one_below, two_below = held
            fix = jnp.where(edge, pltpu.roll(mend2, J - 2 - 4 * k, 1), 0.0)
            m.fs[k] = m.fs[k] + fix
            here = m.pp[k + 1] + fix
            m.pp[k + 1] = here
            z = eliminate(jnp.maximum(k - 1, 0), z, here, two_below)
            z = jnp.where(k == 0, 0.0, z)
            one_below = jnp.where(k == 0, (is_first - 1.0) * here, one_below)
            return z, here, one_below

        z, top, under_top = lax.fori_loop(0, L, forward, (zero,) * 3, unroll=32)
        m.pls[step] = top
        group_rows = start(ROWS + step, [(m.pls.at[step], m.plr.at[step], peers[0])])
        eliminate(L - 1, z, above_sign * top, under_top)
        low = m.pp[1]

        def backward(n, y):
            k = L - 1 - n
            y = m.zz[k] + m.gm[k] * y
            m.zz[k] = y
            return y

        y_low = lax.fori_loop(0, L, backward, zero, unroll=8)
        down = y_low - 0.5 * low * own_inv
        up = m.zz[L - 1] + 0.5 * top * up_inv
        if step == 0:
            m.lev[g, 0] = down
            m.lev[g, 1] = up
            group_rows += start(ROWS, [(m.lev.at[g], m.lev.at[g], dev) for dev in peers])
            messages = strips(1, EDGES + 1, (down, up, top))
        else:
            if not last:
                messages = strips(step + 1, EDGES + step + 1, (down, up, top))
            for d in range(3):
                m.lvs[step - 1, d] = m.mix[0, d] * down + m.mix[1, d] * up
            group_rows += start(ROWS + step, [
                (m.lvs.at[step - 1, d], m.lvr.at[step - 1, d], peers[d]) for d in range(3)])
            m.les[step - 1] = up
            extra = remote(m.les.at[step - 1], m.lex.at[step - 1], {"lev": groups - 1 - g},
                           EXTRA + step - 1, step)
            pl.when(middle)(extra.start)

        def plain(k, held):
            before, acc = held
            y = m.zz[k]
            q = m.pp[k + 1] - 0.5 * (y - before)
            m.qs[k] = q
            return y, acc if last else packed(k, q, acc)

        ghost = y_low - (is_first * y_low - m.aa[0] * low)
        unused_y, q_pack = lax.fori_loop(0, L, plain, (ghost, zero), unroll=16)
        if not last:
            for side in range(2):
                for r in range(2):
                    m.xs[step, side, pl.ds(r * L, L), :] = m.qs[:, side_row(side, r), :]
            m.ys[step] = q_pack
            messages += start(EDGES + step + 1, [
                (m.xs.at[step, 0], m.xr.at[step, 1], x_dev[0]),
                (m.xs.at[step, 1], m.xr.at[step, 0], x_dev[1]),
                (m.ys.at[step], m.yr.at[step, 1], y_dev[0]),
                (m.ys.at[step], m.yr.at[step, 0], y_dev[1]),
            ])


        def move(k, _):
            here = ps[k, inner, :]
            fix = jnp.where(edge, pltpu.roll(mend1, J - 2 - 4 * k, 1), 0.0)
            new_u = us[k, inner, :] - 0.25 * (
                ps[k, pl.ds(PAD + 1, I), :] - ps[k, pl.ds(PAD - 1, I), :])
            new_v = vs[k] - 0.25 * (
                pltpu.roll(here, J - 1, 1) - pltpu.roll(here, 1, 1) + fix)
            if last:
                out_u[k] = new_u
                out_v[k] = new_v
            else:
                us[k, inner, :] = new_u
                vs[k] = new_v
            return 0

        lax.fori_loop(0, L, move, 0, unroll=8)
        for end, at in ((0, 0), (1, I - 1)):
            kick = (0.25 - 0.5 * end) * m.hx[end]
            if last:
                out_u[:, at, :] = out_u[:, at, :] + kick
            else:
                us[:, PAD + at, :] = us[:, PAD + at, :] + kick

        if step == 0:
            arrive(m.recv_sem.at[STATIC], static)
            sta = m.sta
            rows_of = inverse(sta[1, 0] + sta[0, 2], sta[2, 0] + sta[1, 2], sta[3, 0] + sta[2, 2],
                              sta[1, 1], sta[2, 1])
            for slot in range(2):
                face = g + slot
                row = [face_row(rows_of, col, face) for col in range(3)]
                for col in range(3):
                    m.inv[slot, col] = row[col]
                mine = jnp.where((face >= 1) & (face <= 3), 1.0, 0.0).astype(jnp.float32)

                def of(h):
                    return jnp.where(h == 1, row[0], jnp.where(h == 2, row[1], row[2]))

                for d in range(3):
                    o = lax.rem(g + groups - 1 - d, groups)
                    m.cw[slot, d] = jnp.where(o == 0, -row[0], jnp.where(
                        o == groups - 1, row[2], jnp.where(middle, of(o), mine)))
                m.cw[slot, 3] = jnp.where(g == 0, 0.0, of(g))
                m.cw[slot, 4] = jnp.where(g == groups - 1, 0.0, -of(g + 1))
                m.cw[slot, 5] = jnp.where(middle, -of(groups - g), 0.0)
            for d in range(3):
                to = lax.rem(g + 1 + d, groups)
                row = [jnp.where(to == 0, rows_of[0][col], rows_of[2][col]) for col in range(3)]
                raw = (to == 1) | (to == 2)
                m.mix[0, d] = jnp.where(g == 0, 0.0, jnp.where((g == groups - 1) | raw, 1.0, jnp.where(
                    g == 1, row[0], row[1])))
                m.mix[1, d] = jnp.where(g == 0, 1.0, jnp.where((g == groups - 1) | raw, 0.0, jnp.where(
                    g == 1, -row[1], -row[2])))
            for side in range(2):
                part = lambda h, n: x_rows(0, side, h, n)
                rows_of = inverse(part(1, 0) + part(0, 2), part(2, 0) + part(1, 2),
                                  part(3, 0) + part(2, 2), part(1, 1), part(2, 1))
                for slot in range(2):
                    for col in range(3):
                        m.nx[side, 3 * slot + col, 0:2, :] = face_row(rows_of, col, g + slot)
            tiles = [y_tile(0, h) for h in range(groups)]
            part = lambda h, n: jnp.where(live8, turn8(tiles[h], n), 1.0)
            rows_of = inverse(part(1, 0) + part(0, 2), part(2, 0) + part(1, 2),
                              part(3, 0) + part(2, 2), part(1, 1), part(2, 1))
            for slot in range(2):
                for col in range(3):
                    m.ny[3 * slot + col] = jnp.where(live8, face_row(rows_of, col, g + slot), 0.0)
            m.am2[...] = swapped(jnp.where(sub < 2, m.yra[0, 0], m.yra[1, 0]))
            m.bm2[...] = swapped(jnp.where(sub < 2, m.yra[0, 1], m.yra[1, 1]))

        arrive(m.recv_sem.at[ROWS + step], group_rows)
        if step == 0:
            jumps = [m.lev[h, 0] - m.lev[h - 1, 1] for h in (1, 2, 3)]
            under = sum(m.inv[0, n] * jumps[n] for n in range(3))
            over = sum(m.inv[1, n] * jumps[n] for n in range(3))
        else:
            pl.when(middle)(extra.wait)
            terms = [m.lvr[step - 1, d] for d in range(3)] + [down, up, m.lex[step - 1]]
            under = sum(m.cw[0, n] * terms[n] for n in range(6))
            over = sum(m.cw[1, n] * terms[n] for n in range(6))
        under0 = under + 0.5 * m.plr[step]

        def correct(k, acc):
            x = m.zz[k] - m.gf[k] * under + m.gl[k] * over
            new = m.qs[k] + m.aa[k] * jnp.where(k == 0, under0, under) + m.bb[k] * over
            if last:
                out_w[k] = x
                out_p[k] = new
                return acc
            ws[k] = x
            ps[k, inner, :] = new
            return packed(k, new, acc)

        pack = lax.fori_loop(0, L, correct, zero, unroll=32)
        if not last:
            lax.fori_loop(0, L, functools.partial(predict, step + 1), 0, unroll=32)

    arrive(m.send_sem.at[0], sum(rows_sent))


def store_kernel(*refs):
    sem = refs[-1]
    copies = [
        pltpu.make_async_copy(refs[n], refs[4 + n], sem.at[n]) for n in range(4)
    ]
    for copy in copies:
        copy.start()
    for copy in copies:
        copy.wait()


def body(zonal, meridional, vertical, pressure, coupling, surface, lid_flag):
    L, I, J = zonal.shape
    IP = I + 2 * PAD
    S = SUBSTEPS
    G = GROUPS
    f32 = jnp.float32
    V = lambda *shape: pltpu.VMEM(shape, f32)
    level = (L, I, J)
    scratch = dict(
        us=V(L, IP, J), vs=V(*level), ws=V(*level), ps=V(L, IP, J), cs=V(L + 1, I, J),
        ks=pltpu.VMEM((I, J), jnp.int32), ls=pltpu.VMEM((I, J), jnp.int32),
        fs=V(*level), pp=V(L + 2, I, J), zz=V(*level), qs=V(*level),
        am=V(*level), im=V(*level), gm=V(*level), gf=V(*level), gl=V(*level),
        aa=V(*level), bb=V(*level),
        xs0=V(2, 3 * L, J), ys0=V(2, I, J), xr0=V(2, 3 * L, J), yr0=V(2, 2, I, J),
        xs=V(S - 1, 2, 2 * L, J), ys=V(S - 1, I, J),
        xr=V(S - 1, 2, 2 * L, J), yr=V(S - 1, 2, I, J),
        xsa=V(2, 4 * L, J), ysa=V(2, I, J), xra=V(2, 4 * L, J), yra=V(2, 2, I, J),
        xsi=V(S, 2, 6, J), ysi=V(S, 4, J), xri=V(S, 2, G, 6, J), yri=V(S, 2, G, 4, J),
        sta=V(G, 3, I, J), lev=V(G, 2, I, J), cup=V(I, J),
        lvs=V(S - 1, 3, I, J), lvr=V(S - 1, 3, I, J), les=V(S - 1, I, J), lex=V(S - 1, I, J),
        mix=V(2, 3, I, J), cw=V(2, 6, I, J), pls=V(S, I, J), plr=V(S, I, J), hx=V(2, L, J),
        inv=V(2, 3, I, J), nx=V(2, 6, 8, J), ny=V(6, 8, J), am2=V(I, J), bm2=V(I, J),
        sel=pltpu.VMEM((J, 4 * J), jnp.bfloat16),
        load_sem=pltpu.SemaphoreType.DMA((7,)),
        tally=V(2560, J), hood=pltpu.SemaphoreType.REGULAR,
        send_sem=pltpu.SemaphoreType.DMA((S,)),
        recv_sem=pltpu.SemaphoreType.DMA((STATIC + 1,)),
    )
    any_spec = pl.BlockSpec(memory_space=pl.ANY)
    vmem_spec = pl.BlockSpec(memory_space=pltpu.VMEM)
    field = jax.ShapeDtypeStruct(level, f32)
    results = pl.pallas_call(
        functools.partial(kernel, tuple(scratch)),
        out_shape=(V(*level),) * 4,
        in_specs=[any_spec] * 7,
        out_specs=(vmem_spec,) * 4,
        scratch_shapes=list(scratch.values()),
        compiler_params=pltpu.CompilerParams(collective_id=0, has_side_effects=True),
    )(zonal, meridional, vertical, pressure, coupling, surface, lid_flag)
    return tuple(pl.pallas_call(
        store_kernel,
        out_shape=(field,) * 4,
        in_specs=[vmem_spec] * 4,
        out_specs=(any_spec,) * 4,
        scratch_shapes=[pltpu.SemaphoreType.DMA((4,))],
        compiler_params=pltpu.CompilerParams(vmem_limit_bytes=1 << 22),
    )(*results))


def solution(mesh):
    field = P("lev", "gx", "gy")
    plane = P("gx", "gy")
    return jax.shard_map(
        body, mesh=mesh,
        in_specs=(field,) * 5 + (plane,) * 2,
        out_specs=(field,) * 4,
        check_vma=False,
    )
```

```python
import functools
import types

import jax
import jax.numpy as jnp
from jax import lax
from jax.experimental import pallas as pl
from jax.experimental.pallas import tpu as pltpu
from jax.sharding import PartitionSpec as P

SUBSTEPS = 3
MESH = pl.DeviceIdType.MESH
PAD = 8
GROUPS = 4
FAR_FIRST = (1, 0, 2)
EDGES = FIRST = 0
ROWS = EDGES + SUBSTEPS
EXTRA = ROWS + SUBSTEPS
STATIC = EXTRA + SUBSTEPS - 1


def inverse(d1, d2, d3, q1, q2):
    m1 = d2 * d3 - q2 * q2
    whole = 1.0 / (d1 * m1 - q1 * q1 * d3)
    n12 = q1 * d3 * whole
    n13 = q1 * q2 * whole
    n23 = d1 * q2 * whole
    return (
        (m1 * whole, n12, n13),
        (n12, d1 * d3 * whole, n23),
        (n13, n23, (d1 * d2 - q1 * q1) * whole),
    )


def face_row(rows, col, face):
    return jnp.where(face == 1, rows[0][col], jnp.where(
        face == 2, rows[1][col], jnp.where(face == 3, rows[2][col], 0.0)))


def kernel(names, zon, mer, ver, pre, cou, sur, lid, out_u, out_v, out_w, out_p, *scratch):
    m = types.SimpleNamespace(**dict(zip(names, scratch)))
    us, vs, ws, ps, cs = m.us, m.vs, m.ws, m.ps, m.cs
    L, I, J = zon.shape
    g = lax.axis_index("lev")
    gx = lax.axis_index("gx")
    gy = lax.axis_index("gy")
    nx = lax.axis_size("gx")
    ny = lax.axis_size("gy")
    groups = GROUPS
    x_dev = ({"gx": lax.rem(gx + nx - 1, nx)}, {"gx": lax.rem(gx + 1, nx)})
    y_dev = ({"gy": lax.rem(gy + ny - 1, ny)}, {"gy": lax.rem(gy + 1, ny)})
    peers = [{"lev": lax.rem(g + d, groups)} for d in range(1, groups)]
    around = [{**dev, "lev": lax.rem(g + d, groups)}
              for d in range(groups) for dev in x_dev + y_dev]
    inner = pl.ds(PAD, I)

    loads = [
        pltpu.make_async_copy(src, dst, m.load_sem.at[n])
        for n, (src, dst) in enumerate([
            (pre, ps.at[:, inner, :]),
            (mer, vs),
            (zon, us.at[:, inner, :]),
            (cou, cs.at[pl.ds(0, L)]),
            (sur, m.ks),
            (lid, m.ls),
            (ver, ws),
        ])
    ]
    barrier = pltpu.get_barrier_semaphore()
    near = around[:4] + peers
    for dev in near:
        pl.semaphore_signal(barrier, inc=1, device_id=dev, device_id_type=MESH)
    for copy in loads:
        copy.start()

    lane = lax.broadcasted_iota(jnp.int32, (I, J), 1)
    level = lax.broadcasted_iota(jnp.int32, (L, J), 0)
    quad = lane // 4
    sub = lane % 4
    edge = (lane < 2) | (lane >= J - 2)
    lane8 = lax.broadcasted_iota(jnp.int32, (8, J), 1)
    quad8 = lane8 // 4
    lane4 = lax.broadcasted_iota(jnp.int32, (4, J), 1)
    live8 = (quad8 % 4 == 0) & (quad8 < 16)
    zero = jnp.zeros((I, J), jnp.float32)
    def remote(src, dst, dev, slot, send=0):
        return pltpu.make_async_remote_copy(
            src_ref=src, dst_ref=dst, send_sem=m.send_sem.at[send], recv_sem=m.recv_sem.at[slot],
            device_id=dev, device_id_type=MESH)

    middle = (g == 1) | (g == 2)
    rows_sent = []

    def count(ref):
        rows = 1
        for size in ref.shape[:-1]:
            rows *= size
        return rows

    def start(slot, copies):
        rows = 0
        for src, dst, dev in copies:
            remote(src, dst, dev, slot).start()
            rows += count(src)
        rows_sent.append(rows)
        return rows

    def arrive(sem, rows):
        block = m.tally.at[pl.ds(0, rows)]
        pltpu.make_async_copy(block, block, sem).wait()

    def side_row(side, r):
        return r if side == 0 else I - 2 + r

    def packed(k, plane, held):
        return jnp.where(quad == k, pltpu.roll(plane, 4 * k + 2, 1), held)

    def swapped(held):
        return jnp.where(sub < 2, pltpu.roll(held, J - 2, 1), pltpu.roll(held, 2, 1))

    def strips(phase, slot, planes):
        tile = jnp.zeros((8, J), jnp.float32)
        for n, plane in enumerate(planes):
            m.xsi[phase, 0, pl.ds(2 * n, 2), :] = plane[0:2]
            m.xsi[phase, 1, pl.ds(2 * n, 2), :] = plane[I - 2:I]
            for v in range(4):
                turned = pltpu.roll(plane[8 * v:8 * v + 8], 16 * v + 4 * n + 2, 1)
                tile = jnp.where(quad8 == 4 * v + n, turned, tile)
        m.ysi[phase] = jnp.where(lane4 < 64, tile[0:4], pltpu.roll(tile[4:8], 64, 1))
        return start(slot, [
            copy
            for d in (2, 1, 3, 0) for side in range(2)
            for copy in (
                (m.xsi.at[phase, side], m.xri.at[phase, 1 - side, g], around[4 * d + side]),
                (m.ysi.at[phase], m.yri.at[phase, 1 - side, g], around[4 * d + 2 + side]),
            )
        ])

    def x_rows(phase, side, h, n):
        return m.xri[phase, side, h, pl.ds(2 * n, 2), :]

    def y_tile(phase, h):
        half = jnp.where(lane4 % 4 < 2, m.yri[phase, 0, h], m.yri[phase, 1, h])
        return jnp.concatenate([half, pltpu.roll(half, 64, 1)], 0)

    def turn8(tile, n):
        return pltpu.roll(tile, J - 4 * n, 1) if n else tile

    for step in range(SUBSTEPS - 1):
        m.lex[step] = zero
    loads[0].wait()
    for side in range(2):
        for r in range(2):
            m.xs0[side, pl.ds(r * L, L), :] = ps[:, PAD + side_row(side, r), :]
    pack = lax.fori_loop(0, L, lambda k, acc: packed(k, ps[k, inner, :], acc), zero, unroll=32)
    loads[1].wait()
    pack_v = lax.fori_loop(0, L, lambda k, acc: packed(k, vs[k], acc), zero, unroll=32)
    v_up = pltpu.roll(pack_v, 1, 1)
    m.ys0[0] = jnp.where(sub < 2, pltpu.roll(pack, J - 2, 1), pack_v)
    m.ys0[1] = jnp.where(sub < 2, pack, v_up)
    loads[2].wait()
    for side in range(2):
        m.xs0[side, pl.ds(2 * L, L), :] = us[:, PAD + (I - 1) * side, :]
    for n in range(3, 6):
        loads[n].wait()

    pl.semaphore_wait(barrier, len(near))
    for dev in around[:4]:
        pl.semaphore_signal(m.hood, inc=1, device_id=dev, device_id_type=MESH)
    messages = start(FIRST, [
        (m.xs0.at[0], m.xr0.at[1], x_dev[0]),
        (m.xs0.at[1], m.xr0.at[0], x_dev[1]),
        (m.ys0.at[0], m.yr0.at[1], y_dev[0]),
        (m.ys0.at[1], m.yr0.at[0], y_dev[1]),
        (cs.at[0], m.cup, peers[-1]),
    ])

    halo_rows = jnp.zeros((L, PAD, J), jnp.float32)
    for ref in (ps, us):
        ref[:, 0:PAD, :] = halo_rows
        ref[:, PAD + I:, :] = halo_rows

    cs[L] = zero
    height = m.ks[...] - g * L
    lid_here = jnp.where(g == groups - 1, m.ls[...].astype(jnp.float32), 0.0)
    is_first = jnp.where(g == 0, 1.0, 0.0).astype(jnp.float32)
    above_sign = jnp.where(g == groups - 1, 0.0, -1.0).astype(jnp.float32)
    g_below = lax.rem(g + groups - 1, groups)

    def factor(k, held):
        rate, z = held
        here = cs[k]
        above = cs[k + 1]
        keep = height <= k
        delta = 1.0 + here * rate + jnp.where(k == L - 1, lid_here * here, 0.0)
        one = 1.0 / (delta + above)
        rate = jnp.where(keep, delta * one, 1.0)
        one = jnp.where(keep, one, 0.0)
        a = here * one
        z = jnp.where(k == 0, one, a * z)
        m.im[k] = one
        m.am[k] = a
        m.gm[k] = above * one
        m.gf[k] = z
        return rate, z

    lax.fori_loop(0, L, factor, (zero + is_first, zero), unroll=4)

    def respond(n, held):
        a, b = held
        k = L - 1 - n
        up = m.gm[k]
        a = m.gf[k] + up * a
        b = jnp.where(n == 0, m.im[L - 1], up * b)
        m.gf[k] = a
        m.gl[k] = b
        return a, b

    lax.fori_loop(0, L, respond, (zero, zero), unroll=4)
    own_inv = 1.0 / cs[0]
    own_static = (m.gf[0] + own_inv, m.gf[L - 1], m.gl[L - 1])
    for n in range(3):
        m.sta[g, n] = own_static[n]
    static = start(STATIC, [(m.sta.at[g], m.sta.at[g], peers[d]) for d in FAR_FIRST])


    def slopes(k, held):
        f_before, l_before, a_pack, b_pack = held
        f = m.gf[k]
        l = m.gl[k]
        a = jnp.where(k == 0, (is_first - 1.0) * 0.5 * own_inv, 0.5 * (f - f_before))
        b = jnp.where(k == 0, is_first * -0.5 * l, -0.5 * (l - l_before))
        m.aa[k] = a
        m.bb[k] = b
        return f, l, packed(k, a, a_pack), packed(k, b, b_pack)

    unused_f, unused_l, a_pack, b_pack = lax.fori_loop(0, L, slopes, (zero,) * 4, unroll=8)
    m.ysa[0] = a_pack
    m.ysa[1] = b_pack
    for side in range(2):
        for r in range(2):
            m.xsa[side, pl.ds(r * L, L), :] = m.aa[:, side_row(side, r), :]
            m.xsa[side, pl.ds((2 + r) * L, L), :] = m.bb[:, side_row(side, r), :]
    static += start(STATIC, [
        (m.xsa.at[0], m.xra.at[1], x_dev[0]),
        (m.xsa.at[1], m.xra.at[0], x_dev[1]),
        (m.ysa, m.yra.at[1], y_dev[0]),
        (m.ysa, m.yra.at[0], y_dev[1]),
    ])

    pick = lax.broadcasted_iota(jnp.int32, (J, 4 * J), 0)
    into = lax.broadcasted_iota(jnp.int32, (J, 4 * J), 1)
    m.sel[...] = jnp.where(
        (pick % 16 == (into + 2) % 4) & (pick // 16 == into // J), 1.0, 0.0).astype(jnp.bfloat16)

    def predict(step, k, _):
        here = ps[k, inner, :]
        force = 0.0625 * (
            ps[k, pl.ds(PAD + 2, I), :] + ps[k, pl.ds(PAD - 2, I), :]
            + pltpu.roll(here, J - 2, 1) + pltpu.roll(here, 2, 1) - 4.0 * here)
        if step == 0:
            v = vs[k]
            force = force - 0.25 * (
                us[k, pl.ds(PAD + 1, I), :] - us[k, pl.ds(PAD - 1, I), :]
                + pltpu.roll(v, J - 1, 1) - pltpu.roll(v, 1, 1))
        else:
            force = force + m.fs[k]
        m.fs[k] = force
        m.pp[k + 1] = here + force
        return 0

    lax.fori_loop(0, L, functools.partial(predict, 0), 0, unroll=16)
    loads[6].wait()
    pl.semaphore_wait(m.hood, 4)
    static += strips(0, STATIC, [m.sta[g, n] for n in range(3)])

    up_inv = zero
    for step in range(SUBSTEPS):
        last = step == SUBSTEPS - 1
        arrive(m.recv_sem.at[EDGES + step], messages)
        rows = []
        if step == 0:
            for side in range(2):
                rows += [m.xr0[side, pl.ds(r * L, L), :] for r in range(2)]
            diff = jnp.where(sub < 2, m.yr0[1], pltpu.roll(m.yr0[0], 2, 1)) - swapped(pack)
            spin = jnp.where(sub == 1, pltpu.roll(m.yr0[1] - pack_v, J - 1, 1),
                             jnp.where(sub == 2, v_up - m.yr0[0], 0.0))
            up_inv = 1.0 / m.cup[...]
        else:
            for side in range(2):
                jumps = [x_rows(step, side, h, 0) - x_rows(step, side, h - 1, 1) for h in (1, 2, 3)]
                lower = sum(m.nx[side, n, 0:2, :] * jumps[n] for n in range(3))
                upper = sum(m.nx[side, 3 + n, 0:2, :] * jumps[n] for n in range(3))
                floor = lower + 0.5 * x_rows(step, side, g_below, 2)
                for r in range(2):
                    low_r = jnp.where(level == 0, floor[r:r + 1], lower[r:r + 1])
                    rows.append(
                        m.xr[step - 1, side, pl.ds(r * L, L), :]
                        + m.xra[side, pl.ds(r * L, L), :] * low_r
                        + m.xra[side, pl.ds((2 + r) * L, L), :] * upper[r:r + 1])
            tiles = [y_tile(step, h) for h in range(groups)]
            jumps = [tiles[h] - turn8(tiles[h - 1], 1) for h in (1, 2, 3)]
            lower = sum(m.ny[n] * jumps[n] for n in range(3))
            upper = sum(m.ny[3 + n] * jumps[n] for n in range(3))
            floor = jnp.where(live8, lower + 0.5 * turn8(y_tile(step, g_below), 2), 0.0)
            whole = jnp.concatenate([lower, upper, floor], 0)
            coarse = whole.astype(jnp.bfloat16).astype(jnp.float32)
            second = (whole - coarse).astype(jnp.bfloat16).astype(jnp.float32)
            pieces = jnp.concatenate([whole - coarse - second, second, coarse], 0)
            wide = jnp.dot(pieces.astype(jnp.bfloat16), m.sel[...], preferred_element_type=jnp.float32)
            wide = wide[0:24] + wide[24:48] + wide[48:72]
            parts = [jnp.concatenate([wide[8 * n:8 * n + 8, J * v:J * v + J] for v in range(4)], 0)
                     for n in range(3)]
            diff = (swapped(jnp.where(sub < 2, m.yr[step - 1, 0], m.yr[step - 1, 1]) - pack)
                    + m.am2[...] * jnp.where(quad == 0, parts[2], parts[0])
                    + m.bm2[...] * parts[1])
        mend2 = 0.0625 * diff
        mend1 = jnp.where(sub == 1, pltpu.roll(diff, 1, 1),
                          jnp.where(sub == 2, -pltpu.roll(diff, J - 1, 1), 0.0))
        adds = [0.0625 * row for row in rows]
        if step == 0:
            mend2 = mend2 - 0.25 * spin
            adds[0] = adds[0] + 0.25 * m.xr0[0, pl.ds(2 * L, L), :]
            adds[3] = adds[3] - 0.25 * m.xr0[1, pl.ds(2 * L, L), :]
        for at, add in zip((0, 1, I - 2, I - 1), adds):
            m.fs[:, at, :] = m.fs[:, at, :] + add
            m.pp[pl.ds(1, L), at, :] = m.pp[pl.ds(1, L), at, :] + add
        m.hx[0] = rows[1]
        m.hx[1] = rows[2]

        def eliminate(k, z, mid_above, mid_below):
            z = (ws[k] - 0.5 * (mid_above - mid_below)) * m.im[k] + m.am[k] * z
            m.zz[k] = z
            return z

        def forward(k, held):
            z, one_below, two_below = held
            fix = jnp.where(edge, pltpu.roll(mend2, J - 2 - 4 * k, 1), 0.0)
            m.fs[k] = m.fs[k] + fix
            here = m.pp[k + 1] + fix
            m.pp[k + 1] = here
            z = eliminate(jnp.maximum(k - 1, 0), z, here, two_below)
            z = jnp.where(k == 0, 0.0, z)
            one_below = jnp.where(k == 0, (is_first - 1.0) * here, one_below)
            return z, here, one_below

        z, top, under_top = lax.fori_loop(0, L, forward, (zero,) * 3, unroll=32)
        m.pls[step] = top
        group_rows = start(ROWS + step, [(m.pls.at[step], m.plr.at[step], peers[0])])
        eliminate(L - 1, z, above_sign * top, under_top)
        low = m.pp[1]

        def backward(n, y):
            k = L - 1 - n
            y = m.zz[k] + m.gm[k] * y
            m.zz[k] = y
            return y

        y_low = lax.fori_loop(0, L, backward, zero, unroll=8)
        down = y_low - 0.5 * low * own_inv
        up = m.zz[L - 1] + 0.5 * top * up_inv
        if step == 0:
            m.lev[g, 0] = down
            m.lev[g, 1] = up
            group_rows += start(ROWS, [(m.lev.at[g], m.lev.at[g], peers[d]) for d in FAR_FIRST])
            messages = strips(1, EDGES + 1, (down, up, top))
        else:
            if not last:
                messages = strips(step + 1, EDGES + step + 1, (down, up, top))
            for d in range(3):
                m.lvs[step - 1, d] = m.mix[0, d] * down + m.mix[1, d] * up
            group_rows += start(ROWS + step, [
                (m.lvs.at[step - 1, d], m.lvr.at[step - 1, d], peers[d]) for d in FAR_FIRST])
            m.les[step - 1] = up
            extra = remote(m.les.at[step - 1], m.lex.at[step - 1], {"lev": groups - 1 - g},
                           EXTRA + step - 1, step)
            pl.when(middle)(extra.start)

        def plain(k, held):
            before, acc = held
            y = m.zz[k]
            q = m.pp[k + 1] - 0.5 * (y - before)
            m.qs[k] = q
            return y, acc if last else packed(k, q, acc)

        ghost = y_low - (is_first * y_low - m.aa[0] * low)
        unused_y, q_pack = lax.fori_loop(0, L, plain, (ghost, zero), unroll=32)
        if not last:
            for side in range(2):
                for r in range(2):
                    m.xs[step, side, pl.ds(r * L, L), :] = m.qs[:, side_row(side, r), :]
            m.ys[step] = q_pack
            messages += start(EDGES + step + 1, [
                (m.xs.at[step, 0], m.xr.at[step, 1], x_dev[0]),
                (m.xs.at[step, 1], m.xr.at[step, 0], x_dev[1]),
                (m.ys.at[step], m.yr.at[step, 1], y_dev[0]),
                (m.ys.at[step], m.yr.at[step, 0], y_dev[1]),
            ])


        def move(k, _):
            here = ps[k, inner, :]
            fix = jnp.where(edge, pltpu.roll(mend1, J - 2 - 4 * k, 1), 0.0)
            new_u = us[k, inner, :] - 0.25 * (
                ps[k, pl.ds(PAD + 1, I), :] - ps[k, pl.ds(PAD - 1, I), :])
            new_v = vs[k] - 0.25 * (
                pltpu.roll(here, J - 1, 1) - pltpu.roll(here, 1, 1) + fix)
            if last:
                out_u[k] = new_u
                out_v[k] = new_v
            else:
                us[k, inner, :] = new_u
                vs[k] = new_v
            return 0

        lax.fori_loop(0, L, move, 0, unroll=8)
        for end, at in ((0, 0), (1, I - 1)):
            kick = (0.25 - 0.5 * end) * m.hx[end]
            if last:
                out_u[:, at, :] = out_u[:, at, :] + kick
            else:
                us[:, PAD + at, :] = us[:, PAD + at, :] + kick

        if step == 0:
            arrive(m.recv_sem.at[STATIC], static)
            sta = m.sta
            rows_of = inverse(sta[1, 0] + sta[0, 2], sta[2, 0] + sta[1, 2], sta[3, 0] + sta[2, 2],
                              sta[1, 1], sta[2, 1])
            for slot in range(2):
                face = g + slot
                row = [face_row(rows_of, col, face) for col in range(3)]
                for col in range(3):
                    m.inv[slot, col] = row[col]
                mine = jnp.where((face >= 1) & (face <= 3), 1.0, 0.0).astype(jnp.float32)

                def of(h):
                    return jnp.where(h == 1, row[0], jnp.where(h == 2, row[1], row[2]))

                for d in range(3):
                    o = lax.rem(g + groups - 1 - d, groups)
                    m.cw[slot, d] = jnp.where(o == 0, -row[0], jnp.where(
                        o == groups - 1, row[2], jnp.where(middle, of(o), mine)))
                m.cw[slot, 3] = jnp.where(g == 0, 0.0, of(g))
                m.cw[slot, 4] = jnp.where(g == groups - 1, 0.0, -of(g + 1))
                m.cw[slot, 5] = jnp.where(middle, -of(groups - g), 0.0)
            for d in range(3):
                to = lax.rem(g + 1 + d, groups)
                row = [jnp.where(to == 0, rows_of[0][col], rows_of[2][col]) for col in range(3)]
                raw = (to == 1) | (to == 2)
                m.mix[0, d] = jnp.where(g == 0, 0.0, jnp.where((g == groups - 1) | raw, 1.0, jnp.where(
                    g == 1, row[0], row[1])))
                m.mix[1, d] = jnp.where(g == 0, 1.0, jnp.where((g == groups - 1) | raw, 0.0, jnp.where(
                    g == 1, -row[1], -row[2])))
            for side in range(2):
                part = lambda h, n: x_rows(0, side, h, n)
                rows_of = inverse(part(1, 0) + part(0, 2), part(2, 0) + part(1, 2),
                                  part(3, 0) + part(2, 2), part(1, 1), part(2, 1))
                for slot in range(2):
                    for col in range(3):
                        m.nx[side, 3 * slot + col, 0:2, :] = face_row(rows_of, col, g + slot)
            tiles = [y_tile(0, h) for h in range(groups)]
            part = lambda h, n: jnp.where(live8, turn8(tiles[h], n), 1.0)
            rows_of = inverse(part(1, 0) + part(0, 2), part(2, 0) + part(1, 2),
                              part(3, 0) + part(2, 2), part(1, 1), part(2, 1))
            for slot in range(2):
                for col in range(3):
                    m.ny[3 * slot + col] = jnp.where(live8, face_row(rows_of, col, g + slot), 0.0)
            m.am2[...] = swapped(jnp.where(sub < 2, m.yra[0, 0], m.yra[1, 0]))
            m.bm2[...] = swapped(jnp.where(sub < 2, m.yra[0, 1], m.yra[1, 1]))

        arrive(m.recv_sem.at[ROWS + step], group_rows)
        if step == 0:
            jumps = [m.lev[h, 0] - m.lev[h - 1, 1] for h in (1, 2, 3)]
            under = sum(m.inv[0, n] * jumps[n] for n in range(3))
            over = sum(m.inv[1, n] * jumps[n] for n in range(3))
        else:
            pl.when(middle)(extra.wait)
            terms = [m.lvr[step - 1, d] for d in range(3)] + [down, up, m.lex[step - 1]]
            under = sum(m.cw[0, n] * terms[n] for n in range(6))
            over = sum(m.cw[1, n] * terms[n] for n in range(6))
        under0 = under + 0.5 * m.plr[step]

        def correct(k, acc):
            x = m.zz[k] - m.gf[k] * under + m.gl[k] * over
            new = m.qs[k] + m.aa[k] * jnp.where(k == 0, under0, under) + m.bb[k] * over
            if last:
                out_w[k] = x
                out_p[k] = new
                return acc
            ws[k] = x
            ps[k, inner, :] = new
            return packed(k, new, acc)

        pack = lax.fori_loop(0, L, correct, zero, unroll=32)
        if not last:
            lax.fori_loop(0, L, functools.partial(predict, step + 1), 0, unroll=32)

    arrive(m.send_sem.at[0], sum(rows_sent))


def store_kernel(*refs):
    sem = refs[-1]
    copies = [
        pltpu.make_async_copy(refs[n], refs[4 + n], sem.at[n]) for n in range(4)
    ]
    for copy in copies:
        copy.start()
    for copy in copies:
        copy.wait()


def body(zonal, meridional, vertical, pressure, coupling, surface, lid_flag):
    L, I, J = zonal.shape
    IP = I + 2 * PAD
    S = SUBSTEPS
    G = GROUPS
    f32 = jnp.float32
    V = lambda *shape: pltpu.VMEM(shape, f32)
    level = (L, I, J)
    scratch = dict(
        us=V(L, IP, J), vs=V(*level), ws=V(*level), ps=V(L, IP, J), cs=V(L + 1, I, J),
        ks=pltpu.VMEM((I, J), jnp.int32), ls=pltpu.VMEM((I, J), jnp.int32),
        fs=V(*level), pp=V(L + 2, I, J), zz=V(*level), qs=V(*level),
        am=V(*level), im=V(*level), gm=V(*level), gf=V(*level), gl=V(*level),
        aa=V(*level), bb=V(*level),
        xs0=V(2, 3 * L, J), ys0=V(2, I, J), xr0=V(2, 3 * L, J), yr0=V(2, I, J),
        xs=V(S - 1, 2, 2 * L, J), ys=V(S - 1, I, J),
        xr=V(S - 1, 2, 2 * L, J), yr=V(S - 1, 2, I, J),
        xsa=V(2, 4 * L, J), ysa=V(2, I, J), xra=V(2, 4 * L, J), yra=V(2, 2, I, J),
        xsi=V(S, 2, 6, J), ysi=V(S, 4, J), xri=V(S, 2, G, 6, J), yri=V(S, 2, G, 4, J),
        sta=V(G, 3, I, J), lev=V(G, 2, I, J), cup=V(I, J),
        lvs=V(S - 1, 3, I, J), lvr=V(S - 1, 3, I, J), les=V(S - 1, I, J), lex=V(S - 1, I, J),
        mix=V(2, 3, I, J), cw=V(2, 6, I, J), pls=V(S, I, J), plr=V(S, I, J), hx=V(2, L, J),
        inv=V(2, 3, I, J), nx=V(2, 6, 8, J), ny=V(6, 8, J), am2=V(I, J), bm2=V(I, J),
        sel=pltpu.VMEM((J, 4 * J), jnp.bfloat16),
        load_sem=pltpu.SemaphoreType.DMA((7,)),
        tally=V(2560, J), hood=pltpu.SemaphoreType.REGULAR,
        send_sem=pltpu.SemaphoreType.DMA((S,)),
        recv_sem=pltpu.SemaphoreType.DMA((STATIC + 1,)),
    )
    any_spec = pl.BlockSpec(memory_space=pl.ANY)
    vmem_spec = pl.BlockSpec(memory_space=pltpu.VMEM)
    field = jax.ShapeDtypeStruct(level, f32)
    results = pl.pallas_call(
        functools.partial(kernel, tuple(scratch)),
        out_shape=(V(*level),) * 4,
        in_specs=[any_spec] * 7,
        out_specs=(vmem_spec,) * 4,
        scratch_shapes=list(scratch.values()),
        compiler_params=pltpu.CompilerParams(collective_id=0, has_side_effects=True),
    )(zonal, meridional, vertical, pressure, coupling, surface, lid_flag)
    return tuple(pl.pallas_call(
        store_kernel,
        out_shape=(field,) * 4,
        in_specs=[vmem_spec] * 4,
        out_specs=(any_spec,) * 4,
        scratch_shapes=[pltpu.SemaphoreType.DMA((4,))],
        compiler_params=pltpu.CompilerParams(vmem_limit_bytes=1 << 22),
    )(*results))


def solution(mesh):
    field = P("lev", "gx", "gy")
    plane = P("gx", "gy")
    return jax.shard_map(
        body, mesh=mesh,
        in_specs=(field,) * 5 + (plane,) * 2,
        out_specs=(field,) * 4,
        check_vma=False,
    )
```
